64 devices in a mesh: dp: 4 (over x, y), sp: 16 (over z, core).
Axes of the slice: x: 2, y: 2, z: 8, core: 2. Of those that a mesh axis runs over, the one named last changes fastest.
The devices are a block of a 4x4x8 slice.
Arguments:
- tokens: bfloat16 [8192, 4096], P(('dp', 'sp')), parts along dimension 0
- w_query: bfloat16 [4096, 8192], replicated
- w_key: bfloat16 [4096, 512], replicated
- w_value: bfloat16 [4096, 512], replicated
- w_out: bfloat16 [8192, 4096], replicated
- w_gate: bfloat16 [4096, 4096], replicated
- w_up: bfloat16 [4096, 4096], replicated
- w_down: bfloat16 [4096, 4096], replicated
- w_router: bfloat16 [4096, 128], replicated
- expert_ids: int32 [8192, 8], P(('dp', 'sp')), parts along dimension 0
Outputs:
- output 1: bfloat16 [8192, 4096], P(('dp', 'sp')), parts along dimension 0
- output 2: bfloat16 [512, 256, 4096], P(('dp', 'sp')), parts along dimension 0
There are 4 independent parts. The reference program is written for one: setup_inputs(seed, part) draws one part's arguments, and reference() takes and returns one part's arrays. A program takes and returns all parts, laid end to end along the dimension named above; an argument that names none is the same for every part.
All inputs are finite; a program needn't handle non-finite values.
Results may differ from the reference program's by a relative error of at most 0.00603084.
Values are sent between devices in bfloat16 or wider.
A program may use at most 768 MiB of HBM per device.

```python
import math
import jax
import jax.numpy as jnp
from jax import lax

HIDDEN = 4096
Q_HEADS = 64
KV_HEADS = 4
HEAD_DIM = 128
N_EXPERTS = 128
TOP_K = 8
GROUP_SIZE = 16
TOKENS_DEV = 128
CAPACITY = 16

SEQ_LEN = GROUP_SIZE * TOKENS_DEV
Q_WIDTH = Q_HEADS * HEAD_DIM
KV_WIDTH = KV_HEADS * HEAD_DIM
GQA_RATIO = Q_HEADS // KV_HEADS
QUERY_BLOCK = min(SEQ_LEN, 16)
BUF_ROWS = N_EXPERTS * GROUP_SIZE * CAPACITY


def normal_weight(rng_key, rows, cols, gain):
    w_scale = gain / math.sqrt(rows)
    return (jax.random.normal(rng_key, (rows, cols), jnp.float32) * w_scale).astype(jnp.bfloat16)


def draw_routing(rng_key):
    bits_key, hot_key = jax.random.split(rng_key)
    noise_bits = jax.random.randint(bits_key, (SEQ_LEN, N_EXPERTS), 0, 65536)
    expert_range = jnp.arange(N_EXPERTS, dtype=jnp.int32)
    scores = noise_bits * N_EXPERTS + expert_range[None, :]
    hot_expert = jnp.repeat(jax.random.randint(hot_key, (GROUP_SIZE,), 0, N_EXPERTS), TOKENS_DEV)
    local_pos = jnp.arange(SEQ_LEN, dtype=jnp.int32) % TOKENS_DEV
    forced = (local_pos[:, None] < CAPACITY) & (hot_expert[:, None] == expert_range[None, :])
    scores = scores + forced.astype(jnp.int32) * (65536 * N_EXPERTS)
    return lax.top_k(scores, TOP_K)[1].astype(jnp.int32)


def setup_inputs(seed: int = 0, part: int = 0) -> dict:
    base_key = jax.random.key(seed)
    w_keys = jax.random.split(base_key, 8)
    part_keys = jax.random.split(jax.random.fold_in(base_key, part), 2)
    score_gain = math.sqrt(max(1.0, math.log(SEQ_LEN / 8.0)))
    tokens = jax.random.normal(part_keys[0], (SEQ_LEN, HIDDEN), jnp.float32).astype(jnp.bfloat16)
    return {
        'tokens': tokens,
        'w_query': normal_weight(w_keys[0], HIDDEN, Q_WIDTH, score_gain),
        'w_key': normal_weight(w_keys[1], HIDDEN, KV_WIDTH, 1.0),
        'w_value': normal_weight(w_keys[2], HIDDEN, KV_WIDTH, 1.0),
        'w_out': normal_weight(w_keys[3], Q_WIDTH, HIDDEN, 2.0),
        'w_gate': normal_weight(w_keys[4], HIDDEN, HIDDEN, 1.0),
        'w_up': normal_weight(w_keys[5], HIDDEN, HIDDEN, 1.0),
        'w_down': normal_weight(w_keys[6], HIDDEN, HIDDEN, 1.0),
        'w_router': normal_weight(w_keys[7], HIDDEN, N_EXPERTS, 1.0),
        'expert_ids': draw_routing(part_keys[1]),
    }


def attention(queries, keys_bf, values_bf):
    queries_f32 = queries.astype(jnp.float32).reshape(SEQ_LEN // QUERY_BLOCK, QUERY_BLOCK, KV_HEADS, GQA_RATIO, HEAD_DIM)
    keys_f32 = keys_bf.astype(jnp.float32).reshape(SEQ_LEN, KV_HEADS, HEAD_DIM)
    values_f32 = values_bf.astype(jnp.float32).reshape(SEQ_LEN, KV_HEADS, HEAD_DIM)
    key_pos = jnp.arange(SEQ_LEN, dtype=jnp.int32)
    inv_scale = 1.0 / math.sqrt(HEAD_DIM)

    def one_block(blk_args):
        q_blk, q_start = blk_args
        scores = jnp.einsum('qkgd,skd->kgqs', q_blk, keys_f32) * inv_scale
        query_pos = q_start + jnp.arange(QUERY_BLOCK, dtype=jnp.int32)
        scores = jnp.where(query_pos[:, None] >= key_pos[None, :], scores, -jnp.inf)
        attn_probs = jax.nn.softmax(scores, axis=-1).astype(jnp.bfloat16).astype(jnp.float32)
        blk_out = jnp.einsum('kgqs,skd->qkgd', attn_probs, values_f32)
        return blk_out.astype(jnp.bfloat16).reshape(QUERY_BLOCK, Q_WIDTH)

    starts = jnp.arange(SEQ_LEN // QUERY_BLOCK, dtype=jnp.int32) * QUERY_BLOCK
    return lax.map(one_block, (queries_f32, starts)).reshape(SEQ_LEN, Q_WIDTH)


def dispatch(hidden, w_router, expert_ids):
    logits = jnp.dot(hidden, w_router, preferred_element_type=jnp.float32)
    gate_vals = jax.nn.sigmoid(jnp.take_along_axis(logits, expert_ids, axis=1))
    pair_expert = expert_ids.reshape(GROUP_SIZE, TOKENS_DEV * TOP_K)
    onehot = (pair_expert[:, :, None] == jnp.arange(N_EXPERTS, dtype=jnp.int32)[None, None, :]).astype(jnp.int32)
    slot_rank = jnp.sum((jnp.cumsum(onehot, axis=1) - onehot) * onehot, axis=2)
    source = jnp.arange(GROUP_SIZE, dtype=jnp.int32)[:, None]
    dest_row = jnp.where(slot_rank < CAPACITY, (pair_expert * GROUP_SIZE + source) * CAPACITY + slot_rank, BUF_ROWS).reshape(-1)
    pair_token = jnp.arange(SEQ_LEN * TOP_K, dtype=jnp.int32) // TOP_K
    slot_token = jnp.zeros((BUF_ROWS,), jnp.int32).at[dest_row].set(pair_token, mode='drop')
    slot_gate = jnp.zeros((BUF_ROWS,), jnp.float32).at[dest_row].set(gate_vals.reshape(-1), mode='drop')
    gathered = hidden[slot_token].astype(jnp.float32) * slot_gate[:, None]
    return gathered.astype(jnp.bfloat16).reshape(N_EXPERTS, GROUP_SIZE * CAPACITY, HIDDEN)


def reference(tokens, w_query, w_key, w_value, w_out, w_gate, w_up, w_down, w_router, expert_ids):
    queries = jnp.dot(tokens, w_query, preferred_element_type=jnp.float32).astype(jnp.bfloat16)
    keys_bf = jnp.dot(tokens, w_key, preferred_element_type=jnp.float32).astype(jnp.bfloat16)
    values_bf = jnp.dot(tokens, w_value, preferred_element_type=jnp.float32).astype(jnp.bfloat16)
    attn_out = attention(queries, keys_bf, values_bf)
    hidden = (tokens.astype(jnp.float32) + jnp.dot(attn_out, w_out, preferred_element_type=jnp.float32)).astype(jnp.bfloat16)
    gate_act = jnp.dot(hidden, w_gate, preferred_element_type=jnp.float32)
    up_act = jnp.dot(hidden, w_up, preferred_element_type=jnp.float32)
    swiglu = (jax.nn.silu(gate_act) * up_act).astype(jnp.bfloat16)
    hidden_out = (hidden.astype(jnp.float32) + jnp.dot(swiglu, w_down, preferred_element_type=jnp.float32)).astype(jnp.bfloat16)
    expert_buf = dispatch(hidden, w_router, expert_ids)
    return hidden_out, expert_buf
```

```python
import functools
import math
import jax
import jax.numpy as jnp
from jax import lax
from jax.experimental import pallas as pl
from jax.experimental.pallas import tpu as pltpu
from jax.sharding import PartitionSpec as P

HEAD_DIM = 128
NT = (((1,), (1,)), ((), ()))


def attention_body(chunk, rows, me_ref, q_ref, k_ref, v_ref, o_ref, m_ref, l_ref, acc_ref):
    tok = q_ref.shape[0]
    heads = q_ref.shape[1] // HEAD_DIM
    per = rows // tok
    me = me_ref[0]
    factor = math.log2(math.e) / math.sqrt(HEAD_DIM)
    m_ref[...] = jnp.full(m_ref.shape, -jnp.inf, jnp.float32)
    l_ref[...] = jnp.zeros(l_ref.shape, jnp.float32)
    acc_ref[...] = jnp.zeros(acc_ref.shape, jnp.float32)

    def step(start, masked):
        keys = k_ref[pl.ds(start, chunk), :]
        vals = v_ref[pl.ds(start, chunk), :]
        for g in range(heads // per):
            q = jnp.concatenate([q_ref[:, (g * per + i) * HEAD_DIM:(g * per + i + 1) * HEAD_DIM] for i in range(per)], axis=0)
            s = lax.dot_general(q, keys, NT, preferred_element_type=jnp.float32) * factor
            if masked:
                pos = me * tok + lax.rem(lax.broadcasted_iota(jnp.int32, s.shape, 0), tok)
                key = start + lax.broadcasted_iota(jnp.int32, s.shape, 1)
                s = jnp.where(key <= pos, s, -jnp.inf)
            sl = pl.ds(g * rows, rows)
            m_old = m_ref[sl, :1]
            m_new = jnp.maximum(m_old, jnp.max(s, axis=1, keepdims=True))
            p = jnp.exp2(s - m_new)
            alpha = jnp.exp2(m_old - m_new)
            part = p[:, :128]
            for i in range(1, chunk // 128):
                part = part + p[:, i * 128:(i + 1) * 128]
            l_ref[sl, :] = l_ref[sl, :] * alpha + part
            acc_ref[sl, :] = acc_ref[sl, :] * alpha + jnp.dot(p.astype(jnp.bfloat16), vals, preferred_element_type=jnp.float32)
            m_ref[sl, :] = jnp.broadcast_to(m_new, (rows, 128))

    full = (me * tok) // chunk

    @pl.loop(0, full)
    def _(c):
        step(pl.multiple_of(c * chunk, chunk), False)

    step(pl.multiple_of(full * chunk, chunk), True)
    for h in range(heads):
        sl = pl.ds(h * tok, tok)
        total = jnp.sum(l_ref[sl, :], axis=1, keepdims=True)
        o_ref[:, h * HEAD_DIM:(h + 1) * HEAD_DIM] = (acc_ref[sl, :] / total).astype(o_ref.dtype)


def attention(me, queries, kv_all, chunk=512, rows=512):
    tok, width = queries.shape
    seq = kv_all.shape[0]
    kv_heads = kv_all.shape[1] // (2 * HEAD_DIM)
    cols = width // kv_heads
    all_rows = tok * cols // HEAD_DIM
    return pl.pallas_call(
        functools.partial(attention_body, chunk, rows),
        out_shape=jax.ShapeDtypeStruct((tok, width), jnp.bfloat16),
        grid_spec=pltpu.PrefetchScalarGridSpec(
            num_scalar_prefetch=1,
            grid=(kv_heads,),
            in_specs=[
                pl.BlockSpec((tok, cols), lambda i, me: (0, i)),
                pl.BlockSpec((seq, HEAD_DIM), lambda i, me: (0, i)),
                pl.BlockSpec((seq, HEAD_DIM), lambda i, me: (0, kv_heads + i)),
            ],
            out_specs=pl.BlockSpec((tok, cols), lambda i, me: (0, i)),
            scratch_shapes=[
                pltpu.VMEM((all_rows, 128), jnp.float32),
                pltpu.VMEM((all_rows, 128), jnp.float32),
                pltpu.VMEM((all_rows, 128), jnp.float32),
            ],
        ),
        cost_estimate=pl.CostEstimate(flops=4 * tok * width * seq, bytes_accessed=4 * tok * width + 2 * kv_all.size, transcendentals=0),
        compiler_params=pltpu.CompilerParams(vmem_limit_bytes=48 * 2 ** 20),
        name='attention',
    )(me, queries, kv_all, kv_all)


def expand_body(cap, rank_ref, gate_ref, h_ref, out_ref):
    n_loc, tok = rank_ref.shape[1:]
    shape = (n_loc, cap, tok)
    slot = lax.broadcasted_iota(jnp.int32, shape, 1).astype(jnp.float32)
    hit = jnp.broadcast_to(rank_ref[0][:, None, :], shape) == slot
    sel = jnp.where(hit, 1.0, 0.0)
    gate = jnp.sum(sel * jnp.broadcast_to(gate_ref[0][:, None, :], shape), axis=2, keepdims=True)
    sel = sel.reshape(n_loc * cap, tok).astype(jnp.bfloat16)
    gate = gate.reshape(n_loc * cap, 1)
    rows = jnp.dot(sel, h_ref[...], preferred_element_type=jnp.float32)
    out_ref[...] = (rows * gate).astype(out_ref.dtype).reshape(out_ref.shape)


def expand(h_all, rank, gate, cap):
    n_src, n_loc, tok = rank.shape
    width = h_all.shape[1]
    return pl.pallas_call(
        functools.partial(expand_body, cap),
        out_shape=jax.ShapeDtypeStruct((n_loc, n_src * cap, width), jnp.bfloat16),
        grid=(n_src,),
        in_specs=[
            pl.BlockSpec((1, n_loc, tok), lambda s: (s, 0, 0)),
            pl.BlockSpec((1, n_loc, tok), lambda s: (s, 0, 0)),
            pl.BlockSpec((tok, width), lambda s: (s, 0)),
        ],
        out_specs=pl.BlockSpec((n_loc, cap, width), lambda s: (0, s, 0)),
        cost_estimate=pl.CostEstimate(flops=2 * n_src * n_loc * cap * tok * width, bytes_accessed=4 * h_all.size, transcendentals=0),
        name='expand',
    )(rank, gate, h_all)


def slot_ranks(expert_ids, n_experts):
    tok = expert_ids.shape[0]
    chosen = jnp.any(expert_ids[:, :, None] == jnp.arange(n_experts, dtype=jnp.int32), axis=1)
    earlier = jnp.tril(jnp.ones((tok, tok), jnp.bfloat16), -1)
    rank = jnp.dot(earlier, chosen.astype(jnp.bfloat16), preferred_element_type=jnp.float32)
    return jnp.where(chosen, rank, -1.0).T


def solution(mesh):
    row_spec = P(('dp', 'sp'), None)
    buf_spec = P(('dp', 'sp'), None, None)
    replicated = P()

    def local_step(tokens, w_query, w_key, w_value, w_out, w_gate, w_up, w_down, w_router, expert_ids):
        f32, bf16 = jnp.float32, jnp.bfloat16
        tok = tokens.shape[0]
        n_grp = mesh.shape['sp']
        n_experts = w_router.shape[1]
        n_loc = n_experts // n_grp
        cap = max(2, (tok * expert_ids.shape[1] // n_experts) * 2)
        me = lax.axis_index('sp').astype(jnp.int32).reshape(1)
        keys = jnp.dot(tokens, w_key, preferred_element_type=f32).astype(bf16)
        values = jnp.dot(tokens, w_value, preferred_element_type=f32).astype(bf16)
        kv_all = lax.all_gather(jnp.concatenate([keys, values], axis=1), 'sp', axis=0, tiled=True)
        queries = jnp.dot(tokens, w_query, preferred_element_type=f32).astype(bf16)
        attn = attention(me, queries, kv_all)
        hidden = (tokens.astype(f32) + jnp.dot(attn, w_out, preferred_element_type=f32)).astype(bf16)
        h_all = lax.all_gather(hidden, 'sp', axis=0, tiled=True)
        rank = slot_ranks(expert_ids, n_experts)
        gate = jax.nn.sigmoid(jnp.dot(hidden, w_router, preferred_element_type=f32)).T
        table = jnp.concatenate([rank.reshape(n_grp, n_loc, tok), gate.reshape(n_grp, n_loc, tok)], axis=1)
        table = lax.all_to_all(table, 'sp', 0, 0, tiled=True)
        gate_act = jnp.dot(hidden, w_gate, preferred_element_type=f32)
        up_act = jnp.dot(hidden, w_up, preferred_element_type=f32)
        swiglu = (jax.nn.silu(gate_act) * up_act).astype(bf16)
        hidden_out = (hidden.astype(f32) + jnp.dot(swiglu, w_down, preferred_element_type=f32)).astype(bf16)
        expert_buf = expand(h_all, table[:, :n_loc], table[:, n_loc:], cap)
        return hidden_out, expert_buf

    return jax.shard_map(local_step, mesh=mesh, in_specs=(row_spec,) + (replicated,) * 8 + (row_spec,), out_specs=(row_spec, buf_spec), check_vma=False)
```

```python
import functools
import math
import jax
import jax.numpy as jnp
from jax import lax
from jax.experimental import pallas as pl
from jax.experimental.pallas import tpu as pltpu
from jax.sharding import PartitionSpec as P

HEAD_DIM = 128
NT = (((1,), (1,)), ((), ()))
MESH = pl.DeviceIdType.MESH
LAG = 3


def attention_body(chunk, rows, me_ref, q_ref, k_ref, v_ref, o_ref, m_ref, l_ref, acc_ref):
    tok = q_ref.shape[0]
    heads = q_ref.shape[1] // HEAD_DIM
    per = rows // tok
    me = me_ref[0]
    factor = math.log2(math.e) / math.sqrt(HEAD_DIM)
    m_ref[...] = jnp.full(m_ref.shape, -jnp.inf, jnp.float32)
    l_ref[...] = jnp.zeros(l_ref.shape, jnp.float32)
    acc_ref[...] = jnp.zeros(acc_ref.shape, jnp.float32)

    def step(start, masked):
        keys = k_ref[pl.ds(start, chunk), :]
        vals = v_ref[pl.ds(start, chunk), :]
        for g in range(heads // per):
            q = jnp.concatenate([q_ref[:, (g * per + i) * HEAD_DIM:(g * per + i + 1) * HEAD_DIM] for i in range(per)], axis=0)
            s = lax.dot_general(q, keys, NT, preferred_element_type=jnp.float32) * factor
            if masked:
                pos = me * tok + lax.rem(lax.broadcasted_iota(jnp.int32, s.shape, 0), tok)
                key = start + lax.broadcasted_iota(jnp.int32, s.shape, 1)
                s = jnp.where(key <= pos, s, -jnp.inf)
            sl = pl.ds(g * rows, rows)
            m_old = m_ref[sl, :1]
            m_new = jnp.maximum(m_old, jnp.max(s, axis=1, keepdims=True))
            p = jnp.exp2(s - m_new)
            alpha = jnp.exp2(m_old - m_new)
            part = p[:, :128]
            for i in range(1, chunk // 128):
                part = part + p[:, i * 128:(i + 1) * 128]
            l_ref[sl, :] = l_ref[sl, :] * alpha + part
            acc_ref[sl, :] = acc_ref[sl, :] * alpha + jnp.dot(p.astype(jnp.bfloat16), vals, preferred_element_type=jnp.float32)
            m_ref[sl, :] = jnp.broadcast_to(m_new, (rows, 128))

    full = (me * tok) // chunk

    @pl.loop(0, full)
    def _(c):
        step(pl.multiple_of(c * chunk, chunk), False)

    step(pl.multiple_of(full * chunk, chunk), True)
    for h in range(heads):
        sl = pl.ds(h * tok, tok)
        total = jnp.sum(l_ref[sl, :], axis=1, keepdims=True)
        o_ref[:, h * HEAD_DIM:(h + 1) * HEAD_DIM] = (acc_ref[sl, :] / total).astype(o_ref.dtype)


def attention(me, queries, kv_all, chunk=512, rows=512):
    tok, width = queries.shape
    seq = kv_all.shape[0]
    kv_heads = kv_all.shape[1] // (2 * HEAD_DIM)
    cols = width // kv_heads
    all_rows = tok * cols // HEAD_DIM
    return pl.pallas_call(
        functools.partial(attention_body, chunk, rows),
        out_shape=jax.ShapeDtypeStruct((tok, width), jnp.bfloat16),
        grid_spec=pltpu.PrefetchScalarGridSpec(
            num_scalar_prefetch=1,
            grid=(kv_heads,),
            in_specs=[
                pl.BlockSpec((tok, cols), lambda i, me: (0, i)),
                pl.BlockSpec((seq, HEAD_DIM), lambda i, me: (0, i)),
                pl.BlockSpec((seq, HEAD_DIM), lambda i, me: (0, kv_heads + i)),
            ],
            out_specs=pl.BlockSpec((tok, cols), lambda i, me: (0, i)),
            scratch_shapes=[
                pltpu.VMEM((all_rows, 128), jnp.float32),
                pltpu.VMEM((all_rows, 128), jnp.float32),
                pltpu.VMEM((all_rows, 128), jnp.float32),
            ],
        ),
        cost_estimate=pl.CostEstimate(flops=4 * tok * width * seq, bytes_accessed=4 * tok * width + 2 * kv_all.size, transcendentals=0),
        compiler_params=pltpu.CompilerParams(vmem_limit_bytes=48 * 2 ** 20),
        name='attention',
    )(me, queries, kv_all, kv_all)


class Ring:
    def __init__(self, n, buf, up_send, down_send, ring_recv, mate_send, mate_recv):
        self.n, self.len, self.chunks = n, n // 2, buf.shape[1]
        self.half = self.chunks // 2
        self.buf, self.up_send, self.down_send = buf, up_send, down_send
        self.ring_recv, self.mate_send, self.mate_recv = ring_recv, mate_send, mate_recv
        self.me = lax.axis_index('sp')
        self.mate = self.me + 1 - 2 * lax.rem(self.me, 2)
        self.up = lax.rem(self.me + 2, n)
        self.down = lax.rem(self.me + n - 2, n)

    def barrier(self):
        sem = pltpu.get_barrier_semaphore()
        for i in range(1, self.n):
            pl.semaphore_signal(sem, inc=1, device_id={'sp': lax.rem(self.me + i, self.n)}, device_id_type=MESH)
        pl.semaphore_wait(sem, self.n - 1)

    def owner(self, delta, base=None):
        return lax.rem((self.me if base is None else base) + 2 * delta, self.n)

    def copy(self, delta, j, send_sem, recv_sem, target):
        piece = self.buf.at[self.owner(delta), j]
        return pltpu.make_async_remote_copy(src_ref=piece, dst_ref=piece, send_sem=send_sem, recv_sem=recv_sem,
                                            device_id={'sp': target}, device_id_type=MESH)

    def up_copy(self, dist, j):
        delta = lax.rem(self.len - dist, self.len)
        return self.copy(delta, j, self.up_send.at[dist, j], self.ring_recv.at[lax.rem(delta + self.len - 1, self.len), j], self.up)

    def down_copy(self, dist, j):
        return self.copy(dist, j, self.down_send.at[dist, j], self.ring_recv.at[dist + 1, j], self.down)

    def mate_copy(self, delta, j):
        return self.copy(delta, j, self.mate_send.at[delta, j], self.mate_recv.at[delta, j], self.mate)

    def wait_ring(self, delta, j):
        self.copy(delta, j, self.mate_send.at[delta, j], self.ring_recv.at[delta, j], self.mate).wait_recv()

    def wait_mate(self, delta, j):
        piece = self.buf.at[self.owner(delta, self.mate), j]
        pltpu.make_async_remote_copy(src_ref=piece, dst_ref=piece, send_sem=self.mate_send.at[delta, j], recv_sem=self.mate_recv.at[delta, j],
                                     device_id={'sp': self.mate}, device_id_type=MESH).wait_recv()

    def send_own(self, j):
        self.up_copy(0, j).start()
        self.down_copy(0, j).start()
        self.mate_copy(0, j).start()

    def step(self, r):
        dist, j = r // self.chunks + 1, lax.rem(r, self.chunks)
        last = 2 * self.chunks
        self.wait_ring(self.len - dist, j)

        @pl.when(r < last + self.half)
        def _():
            self.up_copy(dist, j).start()

        self.mate_copy(self.len - dist, j).start()
        self.wait_ring(dist, j)

        @pl.when((r < last) | (r >= last + self.half))
        def _():
            self.down_copy(dist, j).start()

        self.mate_copy(dist, j).start()

    def far_step(self, i):
        far = self.len // 2
        for j in (i, i + self.half):
            self.wait_ring(far, j)
            self.mate_copy(far, j).start()

    def drain(self):
        far = self.len // 2

        @pl.loop(0, self.chunks)
        def _(j):
            for dist in range(far):
                @pl.when((dist < far - 1) | (j < self.half))
                def _(dist=dist):
                    self.up_copy(dist, j).wait_send()

                @pl.when((dist < far - 1) | (j >= self.half))
                def _(dist=dist):
                    self.down_copy(dist, j).wait_send()
            for delta in range(self.len):
                self.mate_copy(delta, j).wait_send()


def ring_scratch(n, chunks):
    length, far = n // 2, n // 4
    dma = pltpu.SemaphoreType.DMA
    return [dma((far, chunks)), dma((far, chunks)), dma((length, chunks)), dma((length, chunks)), dma((length, chunks))]


class Tiles:
    def __init__(self, slots, sems, groups):
        self.slots, self.sems, self.groups = slots, sems, groups
        self.depth, self.total = slots.shape[0], groups[-1][0]

    def copy(self, tile, slot):
        return pltpu.make_async_copy(tile, self.slots.at[slot], self.sems.at[slot])

    def start(self, t):
        first = 0
        for end, pick in self.groups:
            @pl.when((t >= first) & (t < end))
            def _(first=first, pick=pick):
                for cond, tile in pick(t - first):
                    if cond is None:
                        self.copy(tile, lax.rem(t, self.depth)).start()
                    else:
                        @pl.when(cond)
                        def _(tile=tile):
                            self.copy(tile, lax.rem(t, self.depth)).start()
            first = end

    def prime(self):
        for t in range(self.depth - 1):
            self.start(jnp.int32(t))

    def take(self, t):
        self.start(t + self.depth - 1)
        slot = lax.rem(t, self.depth)
        self.copy(self.groups[0][1](0)[0][1], slot).wait()
        return self.slots.at[slot]


def columns(j, width):
    return pl.ds(pl.multiple_of(j * width, width), width)


def tail_body(n, cap, o_ref, x_ref, rank_ref, router_ref, wo_ref, wg_ref, wu_ref, wd_ref, y_ref, e_ref,
              buf, row_ref, act_ref, slots, table_out, table_in, sems, table_send, table_recv, *ring_sems):
    f32, bf16 = jnp.float32, jnp.bfloat16
    ring = Ring(n, buf, *ring_sems)
    me = ring.me
    chunks, tok, width = buf.shape[1:]
    depth = slots.shape[1]
    parts = o_ref.shape[1] // depth
    n_loc = rank_ref.shape[0] // n
    tiles = Tiles(slots, sems, (
        (parts * chunks, lambda t: [(None, wo_ref.at[columns(lax.rem(t, parts), depth), columns(t // parts, width)])]),
        ((parts + 2) * chunks, lambda t: [(lax.rem(t, 2) == 0, wg_ref.at[:, columns(t // 2, width)]),
                                          (lax.rem(t, 2) == 1, wu_ref.at[:, columns(t // 2, width)])]),
        ((parts + 3) * chunks, lambda t: [(None, wd_ref.at[:, columns(t, width)])]),
    ))
    tiles.prime()
    ring.barrier()

    @pl.loop(0, chunks)
    def _(j):
        acc = x_ref[:, columns(j, width)].astype(f32)
        part = None
        for i in range(parts):
            prod = jnp.dot(o_ref[:, i * depth:(i + 1) * depth], tiles.take(parts * j + i)[...], preferred_element_type=f32)
            part = prod if part is None else part + prod
        h = (acc + part).astype(bf16)
        buf[me, j] = h
        row_ref[:, columns(j, width)] = h
        ring.send_own(j)

        @pl.when(j >= LAG)
        def _():
            ring.step(j - LAG)

    gate = jax.nn.sigmoid(jnp.dot(row_ref[...], router_ref[...], preferred_element_type=f32)).T
    for d in range(n):
        table_out[d, :n_loc] = rank_ref[d * n_loc:(d + 1) * n_loc]
        table_out[d, n_loc:] = gate[d * n_loc:(d + 1) * n_loc]
    table_in[me] = table_out[me]

    def table_copy(i):
        dst = lax.rem(me + i, n)
        return pltpu.make_async_remote_copy(src_ref=table_out.at[dst], dst_ref=table_in.at[me], send_sem=table_send.at[i], recv_sem=table_recv.at[i],
                                            device_id={'sp': dst}, device_id_type=MESH)

    def table_arrival(i):
        src = lax.rem(me + n - i, n)
        return pltpu.make_async_remote_copy(src_ref=table_out.at[src], dst_ref=table_in.at[src], send_sem=table_send.at[i], recv_sem=table_recv.at[i],
                                            device_id={'sp': src}, device_id_type=MESH)

    for i in range(1, n):
        table_copy(i).start()

    base = parts * chunks

    @pl.loop(0, chunks)
    def _(j):
        h = row_ref[...]
        g = jnp.dot(h, tiles.take(base + 2 * j)[...], preferred_element_type=f32)
        u = jnp.dot(h, tiles.take(base + 2 * j + 1)[...], preferred_element_type=f32)
        act_ref[:, columns(j, width)] = (g * jax.nn.sigmoid(g) * u).astype(bf16)
        ring.step(j + chunks - LAG)

    base += 2 * chunks

    @pl.loop(0, chunks)
    def _(j):
        y = jnp.dot(act_ref[...], tiles.take(base + j)[...], preferred_element_type=f32)
        y_ref[:, columns(j, width)] = (row_ref[:, columns(j, width)].astype(f32) + y).astype(bf16)

        @pl.when(lax.rem(j, 2) == 1)
        def _():
            ring.step(2 * chunks - LAG + j // 2)

    for i in range(1, n):
        table_arrival(i).wait_recv()

    def expand(src, js):
        shape = (n_loc, cap, tok)
        table = table_in[src]
        slot = lax.broadcasted_iota(jnp.int32, shape, 1).astype(f32)
        sel = jnp.where(jnp.broadcast_to(table[:n_loc][:, None, :], shape) == slot, 1.0, 0.0)
        scale = jnp.sum(sel * jnp.broadcast_to(table[n_loc:][:, None, :], shape), axis=2, keepdims=True).reshape(n_loc * cap, 1)
        sel = sel.reshape(n_loc * cap, tok).astype(bf16)
        for j in js:
            rows = jnp.dot(sel, buf[src, j], preferred_element_type=f32) * scale
            e_ref[:, pl.ds(pl.multiple_of(src * cap, cap), cap), columns(j, width)] = rows.astype(bf16).reshape(n_loc, cap, width)

    def expand_pair(delta):
        expand(ring.owner(delta), range(chunks))

        @pl.loop(0, chunks)
        def _(j):
            ring.wait_mate(delta, j)

        expand(ring.owner(delta, ring.mate), range(chunks))

    done = 2 * chunks - LAG + chunks // 2
    length, far = n // 2, n // 4
    near = 2 * far - 3

    @pl.loop(0, 3 * chunks - done)
    def _(k):
        ring.step(done + k)

        @pl.when(k < near)
        def _():
            expand_pair(jnp.where(lax.rem(k, 2) == 1, length - (k + 1) // 2, k // 2))

    @pl.loop(0, chunks // 2)
    def _(i):
        ring.far_step(i)

        @pl.when(i < 2)
        def _():
            expand_pair(jnp.where(i == 0, far + 1, far - 1))

    @pl.loop(0, chunks // 2)
    def _(i):
        js = (i, i + chunks // 2)
        expand(ring.owner(far), js)
        for j in js:
            ring.wait_mate(far, j)
        expand(ring.owner(far, ring.mate), js)

    ring.drain()
    for i in range(1, n):
        table_copy(i).wait_send()


def tail(n, cap, attn, tokens, rank, w_router, w_out, w_gate, w_up, w_down, chunks=8, depth=4):
    tok, hidden = tokens.shape
    width = hidden // chunks
    n_loc = rank.shape[0] // n
    vmem = pl.BlockSpec(memory_space=pltpu.VMEM)
    hbm = pl.BlockSpec(memory_space=pl.ANY)
    dma = pltpu.SemaphoreType.DMA
    weights = w_out.size + w_gate.size + w_up.size + w_down.size
    return pl.pallas_call(
        functools.partial(tail_body, n, cap),
        out_shape=(jax.ShapeDtypeStruct((tok, hidden), jnp.bfloat16),
                   jax.ShapeDtypeStruct((n_loc, n * cap, hidden), jnp.bfloat16)),
        in_specs=[vmem] * 4 + [hbm] * 4,
        out_specs=(vmem, vmem),
        scratch_shapes=[
            pltpu.VMEM((n, chunks, tok, width), jnp.bfloat16),
            pltpu.VMEM((tok, hidden), jnp.bfloat16),
            pltpu.VMEM((tok, hidden), jnp.bfloat16),
            pltpu.VMEM((depth, hidden, width), jnp.bfloat16),
            pltpu.VMEM((n, 2 * n_loc, tok), jnp.float32),
            pltpu.VMEM((n, 2 * n_loc, tok), jnp.float32),
            dma((depth,)), dma((n,)), dma((n,)),
        ] + ring_scratch(n, chunks),
        cost_estimate=pl.CostEstimate(flops=2 * tok * weights, bytes_accessed=2 * weights, transcendentals=0),
        compiler_params=pltpu.CompilerParams(vmem_limit_bytes=67043328, collective_id=0, has_side_effects=True),
        name='tail',
    )(attn, tokens, rank, w_router, w_out, w_gate, w_up, w_down)


def slot_ranks(expert_ids, n_experts):
    tok = expert_ids.shape[0]
    chosen = jnp.any(expert_ids[:, :, None] == jnp.arange(n_experts, dtype=jnp.int32), axis=1)
    earlier = jnp.tril(jnp.ones((tok, tok), jnp.bfloat16), -1)
    rank = jnp.dot(earlier, chosen.astype(jnp.bfloat16), preferred_element_type=jnp.float32)
    return jnp.where(chosen, rank, -1.0).T


def solution(mesh):
    row_spec = P(('dp', 'sp'), None)
    buf_spec = P(('dp', 'sp'), None, None)
    replicated = P()

    def local_step(tokens, w_query, w_key, w_value, w_out, w_gate, w_up, w_down, w_router, expert_ids):
        f32, bf16 = jnp.float32, jnp.bfloat16
        tok = tokens.shape[0]
        n_grp = mesh.shape['sp']
        n_experts = w_router.shape[1]
        cap = max(2, (tok * expert_ids.shape[1] // n_experts) * 2)
        me = lax.axis_index('sp').astype(jnp.int32).reshape(1)
        keys = jnp.dot(tokens, w_key, preferred_element_type=f32).astype(bf16)
        values = jnp.dot(tokens, w_value, preferred_element_type=f32).astype(bf16)
        kv_all = lax.all_gather(jnp.concatenate([keys, values], axis=1), 'sp', axis=0, tiled=True)
        queries = jnp.dot(tokens, w_query, preferred_element_type=f32).astype(bf16)
        attn = attention(me, queries, kv_all)
        rank = slot_ranks(expert_ids, n_experts)
        hidden_out, expert_buf = tail(n_grp, cap, attn, tokens, rank, w_router, w_out, w_gate, w_up, w_down)
        return hidden_out, expert_buf

    return jax.shard_map(local_step, mesh=mesh, in_specs=(row_spec,) + (replicated,) * 8 + (row_spec,), out_specs=(row_spec, buf_spec), check_vma=False)
```

```python
import functools
import math
import jax
import jax.numpy as jnp
from jax import lax
from jax.experimental import pallas as pl
from jax.experimental.pallas import tpu as pltpu
from jax.sharding import PartitionSpec as P

HEAD_DIM = 128
NT = (((1,), (1,)), ((), ()))
MESH = pl.DeviceIdType.MESH
LAG = 3


def attention_body(chunk, rows, me_ref, q_ref, k_ref, v_ref, o_ref, m_ref, l_ref, acc_ref, bias_ref):
    tok = q_ref.shape[0]
    heads = q_ref.shape[1] // HEAD_DIM
    per = rows // tok
    blocks = chunk // tok
    me = me_ref[0]
    factor = math.log2(math.e) / math.sqrt(HEAD_DIM)
    full = (me * tok) // chunk
    m_ref[...] = jnp.full(m_ref.shape, -jnp.inf, jnp.float32)
    l_ref[...] = jnp.zeros(l_ref.shape, jnp.float32)
    acc_ref[...] = jnp.zeros(acc_ref.shape, jnp.float32)
    pos = me * tok - full * chunk + lax.broadcasted_iota(jnp.int32, bias_ref.shape, 0)
    key = lax.broadcasted_iota(jnp.int32, bias_ref.shape, 1)
    bias_ref[...] = jnp.where(key <= pos, 0.0, -jnp.inf)

    def step(c, masked):
        keys = k_ref[pl.ds(c * blocks, blocks), 0].reshape(chunk, HEAD_DIM)
        vals = v_ref[pl.ds(c * blocks, blocks), 0].reshape(chunk, HEAD_DIM)
        for g in range(heads // per):
            q = jnp.concatenate([q_ref[:, (g * per + i) * HEAD_DIM:(g * per + i + 1) * HEAD_DIM] for i in range(per)], axis=0)
            s = lax.dot_general(q, keys, NT, preferred_element_type=jnp.float32) * factor
            if masked:
                s = (s.reshape(per, tok, chunk) + bias_ref[...][None]).reshape(rows, chunk)
            sl = pl.ds(g * rows, rows)
            m_old = m_ref[sl, :]
            m_new = jnp.maximum(m_old, jnp.max(s, axis=1, keepdims=True))
            p = jnp.exp2(s - m_new[:, :1])
            alpha = jnp.exp2(m_old - m_new)
            part = p[:, :128]
            for i in range(1, chunk // 128):
                part = part + p[:, i * 128:(i + 1) * 128]
            l_ref[sl, :] = l_ref[sl, :] * alpha + part
            acc_ref[sl, :] = acc_ref[sl, :] * alpha + jnp.dot(p.astype(jnp.bfloat16), vals, preferred_element_type=jnp.float32)
            m_ref[sl, :] = m_new

    @pl.loop(0, full)
    def _(c):
        step(c, False)

    step(full, True)
    for h in range(heads):
        sl = pl.ds(h * tok, tok)
        total = jnp.sum(l_ref[sl, :], axis=1, keepdims=True)
        o_ref[:, h * HEAD_DIM:(h + 1) * HEAD_DIM] = (acc_ref[sl, :] * (1.0 / total)).astype(o_ref.dtype)


def attention(me, queries, kv_all, chunk=512, rows=512):
    tok, width = queries.shape
    n_src, _, _, kv_width = kv_all.shape
    kv_heads = kv_width // HEAD_DIM
    cols = width // kv_heads
    all_rows = tok * cols // HEAD_DIM
    return pl.pallas_call(
        functools.partial(attention_body, chunk, rows),
        out_shape=jax.ShapeDtypeStruct((tok, width), jnp.bfloat16),
        grid_spec=pltpu.PrefetchScalarGridSpec(
            num_scalar_prefetch=1,
            grid=(kv_heads,),
            in_specs=[
                pl.BlockSpec((tok, cols), lambda i, me: (0, i)),
                pl.BlockSpec((n_src, 1, tok, HEAD_DIM), lambda i, me: (0, 0, 0, i)),
                pl.BlockSpec((n_src, 1, tok, HEAD_DIM), lambda i, me: (0, 1, 0, i)),
            ],
            out_specs=pl.BlockSpec((tok, cols), lambda i, me: (0, i)),
            scratch_shapes=[
                pltpu.VMEM((all_rows, 128), jnp.float32),
                pltpu.VMEM((all_rows, 128), jnp.float32),
                pltpu.VMEM((all_rows, 128), jnp.float32),
                pltpu.VMEM((tok, chunk), jnp.float32),
            ],
        ),
        cost_estimate=pl.CostEstimate(flops=4 * tok * width * n_src * tok, bytes_accessed=4 * tok * width + 2 * kv_all.size, transcendentals=0),
        compiler_params=pltpu.CompilerParams(vmem_limit_bytes=40 * 2 ** 20),
        name='attention',
    )(me, queries, kv_all, kv_all)


class Ring:
    def __init__(self, n, buf, up_send, down_send, ring_recv, mate_send, mate_recv):
        self.n, self.len, self.chunks = n, n // 2, buf.shape[1]
        self.half = self.chunks // 2
        self.buf, self.up_send, self.down_send = buf, up_send, down_send
        self.ring_recv, self.mate_send, self.mate_recv = ring_recv, mate_send, mate_recv
        self.me = lax.axis_index('sp')
        self.mate = self.me + 1 - 2 * lax.rem(self.me, 2)
        self.up = lax.rem(self.me + 2, n)
        self.down = lax.rem(self.me + n - 2, n)

    def barrier(self):
        sem = pltpu.get_barrier_semaphore()
        for i in range(1, self.n):
            pl.semaphore_signal(sem, inc=1, device_id={'sp': lax.rem(self.me + i, self.n)}, device_id_type=MESH)
        pl.semaphore_wait(sem, self.n - 1)

    def owner(self, delta, base=None):
        return lax.rem((self.me if base is None else base) + 2 * delta, self.n)

    def copy(self, delta, j, send_sem, recv_sem, target):
        piece = self.buf.at[self.owner(delta), j]
        return pltpu.make_async_remote_copy(src_ref=piece, dst_ref=piece, send_sem=send_sem, recv_sem=recv_sem,
                                            device_id={'sp': target}, device_id_type=MESH)

    def up_copy(self, dist, j):
        delta = lax.rem(self.len - dist, self.len)
        return self.copy(delta, j, self.up_send.at[dist, j], self.ring_recv.at[lax.rem(delta + self.len - 1, self.len), j], self.up)

    def down_copy(self, dist, j):
        return self.copy(dist, j, self.down_send.at[dist, j], self.ring_recv.at[dist + 1, j], self.down)

    def mate_copy(self, delta, j):
        return self.copy(delta, j, self.mate_send.at[delta, j], self.mate_recv.at[delta, j], self.mate)

    def wait_ring(self, delta, j):
        self.copy(delta, j, self.mate_send.at[delta, j], self.ring_recv.at[delta, j], self.mate).wait_recv()

    def wait_mate(self, delta, j):
        piece = self.buf.at[self.owner(delta, self.mate), j]
        pltpu.make_async_remote_copy(src_ref=piece, dst_ref=piece, send_sem=self.mate_send.at[delta, j], recv_sem=self.mate_recv.at[delta, j],
                                     device_id={'sp': self.mate}, device_id_type=MESH).wait_recv()

    def send_own(self, j):
        self.up_copy(0, j).start()
        self.down_copy(0, j).start()
        self.mate_copy(0, j).start()

    def step(self, r):
        dist, j = r // self.chunks + 1, lax.rem(r, self.chunks)
        last = 2 * self.chunks
        self.wait_ring(self.len - dist, j)

        @pl.when(r < last + self.half)
        def _():
            self.up_copy(dist, j).start()

        self.mate_copy(self.len - dist, j).start()
        self.wait_ring(dist, j)

        @pl.when((r < last) | (r >= last + self.half))
        def _():
            self.down_copy(dist, j).start()

        self.mate_copy(dist, j).start()

    def far_step(self, i):
        far = self.len // 2
        for j in (i, i + self.half):
            self.wait_ring(far, j)
            self.mate_copy(far, j).start()

    def drain(self):
        far = self.len // 2

        @pl.loop(0, self.chunks)
        def _(j):
            for dist in range(far):
                @pl.when((dist < far - 1) | (j < self.half))
                def _(dist=dist):
                    self.up_copy(dist, j).wait_send()

                @pl.when((dist < far - 1) | (j >= self.half))
                def _(dist=dist):
                    self.down_copy(dist, j).wait_send()
            for delta in range(self.len):
                self.mate_copy(delta, j).wait_send()


def ring_scratch(n, chunks):
    length, far = n // 2, n // 4
    dma = pltpu.SemaphoreType.DMA
    return [dma((far, chunks)), dma((far, chunks)), dma((length, chunks)), dma((length, chunks)), dma((length, chunks))]


class Tiles:
    def __init__(self, slots, sems, groups):
        self.slots, self.sems, self.groups = slots, sems, groups
        self.depth, self.total = slots.shape[0], groups[-1][0]

    def copy(self, tile, slot):
        return pltpu.make_async_copy(tile, self.slots.at[slot], self.sems.at[slot])

    def start(self, t):
        first = 0
        for end, pick in self.groups:
            @pl.when((t >= first) & (t < end))
            def _(first=first, pick=pick):
                for cond, tile in pick(t - first):
                    if cond is None:
                        self.copy(tile, lax.rem(t, self.depth)).start()
                    else:
                        @pl.when(cond)
                        def _(tile=tile):
                            self.copy(tile, lax.rem(t, self.depth)).start()
            first = end

    def prime(self):
        for t in range(self.depth - 1):
            self.start(jnp.int32(t))

    def take(self, t):
        self.start(t + self.depth - 1)
        slot = lax.rem(t, self.depth)
        self.copy(self.groups[0][1](0)[0][1], slot).wait()
        return self.slots.at[slot]


def columns(j, width):
    return pl.ds(pl.multiple_of(j * width, width), width)


def front_body(n, x_ref, wk_ref, wv_ref, wq_ref, q_ref, kv_ref, buf, slots, sems, out_sem, *ring_sems):
    ring = Ring(n, buf, *ring_sems)
    width = slots.shape[2]
    count = wq_ref.shape[1] // width
    tiles = Tiles(slots, sems, (
        (1, lambda t: [(None, wk_ref)]),
        (2, lambda t: [(None, wv_ref)]),
        (2 + count, lambda t: [(None, wq_ref.at[:, columns(t, width)])]),
    ))
    tiles.prime()
    ring.barrier()
    for c in range(2):
        buf[ring.me, c] = jnp.dot(x_ref[...], tiles.take(jnp.int32(c))[...], preferred_element_type=jnp.float32).astype(jnp.bfloat16)
        ring.send_own(jnp.int32(c))

    steps = 3 * ring.chunks

    @pl.loop(0, count)
    def _(j):
        q_ref[:, columns(j, width)] = jnp.dot(x_ref[...], tiles.take(j + 2)[...], preferred_element_type=jnp.float32).astype(jnp.bfloat16)

        @pl.when((lax.rem(j, 2) == 1) & (j >= 3) & (j < 3 + 2 * steps))
        def _():
            ring.step((j - 3) // 2)

    for r in range(max(0, (count - 2) // 2), steps):
        ring.step(jnp.int32(r))
    ring.far_step(jnp.int32(0))
    for delta in range(ring.len):
        for c in range(2):
            ring.wait_mate(delta, c)
    out = pltpu.make_async_copy(buf, kv_ref, out_sem.at[0])
    out.start()
    ring.drain()
    out.wait()


def front(n, tokens, w_key, w_value, w_query, depth=4):
    tok, hidden = tokens.shape
    width = w_key.shape[1]
    vmem = pl.BlockSpec(memory_space=pltpu.VMEM)
    hbm = pl.BlockSpec(memory_space=pl.ANY)
    dma = pltpu.SemaphoreType.DMA
    weights = w_key.size + w_value.size + w_query.size
    return pl.pallas_call(
        functools.partial(front_body, n),
        out_shape=(jax.ShapeDtypeStruct((tok, w_query.shape[1]), jnp.bfloat16),
                   jax.ShapeDtypeStruct((n, 2, tok, width), jnp.bfloat16)),
        in_specs=[vmem] + [hbm] * 3,
        out_specs=(vmem, hbm),
        scratch_shapes=[
            pltpu.VMEM((n, 2, tok, width), jnp.bfloat16),
            pltpu.VMEM((depth, hidden, width), jnp.bfloat16),
            dma((depth,)), dma((1,)),
        ] + ring_scratch(n, 2),
        cost_estimate=pl.CostEstimate(flops=2 * tok * weights, bytes_accessed=2 * weights, transcendentals=0),
        compiler_params=pltpu.CompilerParams(vmem_limit_bytes=40 * 2 ** 20, collective_id=1, has_side_effects=True),
        name='front',
    )(tokens, w_key, w_value, w_query)


def tail_body(n, cap, o_ref, x_ref, rank_ref, router_ref, wo_ref, wg_ref, wu_ref, wd_ref, y_ref, e_ref,
              buf, row_ref, act_ref, slots, stage, table_out, table_in, sems, stage_sem, table_send, table_recv, *ring_sems):
    f32, bf16 = jnp.float32, jnp.bfloat16
    ring = Ring(n, buf, *ring_sems)
    me = ring.me
    chunks, tok, width = buf.shape[1:]
    depth = slots.shape[1]
    parts = o_ref.shape[1] // depth
    n_loc = rank_ref.shape[0] // n
    tiles = Tiles(slots, sems, (
        (parts * chunks, lambda t: [(None, wo_ref.at[columns(lax.rem(t, parts), depth), columns(t // parts, width)])]),
        ((parts + 2) * chunks, lambda t: [(lax.rem(t, 2) == 0, wg_ref.at[:, columns(t // 2, width)]),
                                          (lax.rem(t, 2) == 1, wu_ref.at[:, columns(t // 2, width)])]),
        ((parts + 3) * chunks, lambda t: [(None, wd_ref.at[:, columns(t, width)])]),
    ))
    tiles.prime()
    ring.barrier()

    @pl.loop(0, chunks)
    def _(j):
        acc = x_ref[:, columns(j, width)].astype(f32)
        part = None
        for i in range(parts):
            prod = jnp.dot(o_ref[:, i * depth:(i + 1) * depth], tiles.take(parts * j + i)[...], preferred_element_type=f32)
            part = prod if part is None else part + prod
        h = (acc + part).astype(bf16)
        buf[me, j] = h
        row_ref[:, columns(j, width)] = h
        ring.send_own(j)

        @pl.when(j >= LAG)
        def _():
            ring.step(j - LAG)

    gate = jax.nn.sigmoid(jnp.dot(row_ref[...], router_ref[...], preferred_element_type=f32)).T
    for d in range(n):
        table_out[d, :n_loc] = rank_ref[d * n_loc:(d + 1) * n_loc]
        table_out[d, n_loc:] = gate[d * n_loc:(d + 1) * n_loc]
    table_in[me] = table_out[me]

    def table_copy(i):
        dst = lax.rem(me + i, n)
        return pltpu.make_async_remote_copy(src_ref=table_out.at[dst], dst_ref=table_in.at[me], send_sem=table_send.at[i], recv_sem=table_recv.at[i],
                                            device_id={'sp': dst}, device_id_type=MESH)

    def table_arrival(i):
        src = lax.rem(me + n - i, n)
        return pltpu.make_async_remote_copy(src_ref=table_out.at[src], dst_ref=table_in.at[src], send_sem=table_send.at[i], recv_sem=table_recv.at[i],
                                            device_id={'sp': src}, device_id_type=MESH)

    for i in range(1, n):
        table_copy(i).start()

    base = parts * chunks

    @pl.loop(0, chunks)
    def _(j):
        h = row_ref[...]
        g = jnp.dot(h, tiles.take(base + 2 * j)[...], preferred_element_type=f32)
        u = jnp.dot(h, tiles.take(base + 2 * j + 1)[...], preferred_element_type=f32)
        act_ref[:, columns(j, width)] = (g * jax.nn.sigmoid(g) * u).astype(bf16)
        ring.step(j + chunks - LAG)

    base += 2 * chunks

    @pl.loop(0, chunks)
    def _(j):
        y = jnp.dot(act_ref[...], tiles.take(base + j)[...], preferred_element_type=f32)
        y_ref[:, columns(j, width)] = (row_ref[:, columns(j, width)].astype(f32) + y).astype(bf16)

        @pl.when(lax.rem(j, 2) == 1)
        def _():
            ring.step(2 * chunks - LAG + j // 2)

    for i in range(1, n):
        table_arrival(i).wait_recv()

    def flush(slot, src):
        return pltpu.make_async_copy(stage.at[slot], e_ref.at[:, pl.ds(pl.multiple_of(src * cap, cap), cap), :], stage_sem.at[slot])

    def expand(slot, src, js):
        shape = (n_loc, cap, tok)
        table = table_in[src]
        place = lax.broadcasted_iota(jnp.int32, shape, 1).astype(f32)
        sel = jnp.where(jnp.broadcast_to(table[:n_loc][:, None, :], shape) == place, 1.0, 0.0)
        scale = jnp.sum(sel * jnp.broadcast_to(table[n_loc:][:, None, :], shape), axis=2, keepdims=True).reshape(n_loc * cap, 1)
        sel = sel.reshape(n_loc * cap, tok).astype(bf16)
        for j in js:
            rows = jnp.dot(sel, buf[src, j], preferred_element_type=f32) * scale
            stage[slot, :, :, columns(j, width)] = rows.astype(bf16).reshape(n_loc, cap, width)

    def expand_pair(delta, first):
        for slot, base in ((0, me), (1, ring.mate)):
            src = ring.owner(delta, base)
            if slot == 1:
                @pl.loop(0, chunks)
                def _(j):
                    ring.wait_mate(delta, j)

            @pl.when(jnp.logical_not(first))
            def _():
                flush(slot, src).wait()
            expand(slot, src, range(chunks))
            flush(slot, src).start()

    done = 2 * chunks - LAG + chunks // 2
    length, far = n // 2, n // 4
    near = 2 * far - 3

    @pl.loop(0, 3 * chunks - done)
    def _(k):
        ring.step(done + k)

        @pl.when(k < near)
        def _():
            expand_pair(jnp.where(lax.rem(k, 2) == 1, length - (k + 1) // 2, k // 2), k == 0)

    @pl.loop(0, chunks // 2)
    def _(i):
        ring.far_step(i)

        @pl.when(i < 2)
        def _():
            expand_pair(jnp.where(i == 0, far + 1, far - 1), i < 0)

    ends = (ring.owner(far), ring.owner(far, ring.mate))
    for slot in range(2):
        flush(slot, ends[slot]).wait()

    @pl.loop(0, chunks // 2)
    def _(i):
        js = (i, i + chunks // 2)
        expand(0, ends[0], js)
        for j in js:
            ring.wait_mate(far, j)
        expand(1, ends[1], js)

    for slot in range(2):
        flush(slot, ends[slot]).start()
    for slot in range(2):
        flush(slot, ends[slot]).wait()
    ring.drain()
    for i in range(1, n):
        table_copy(i).wait_send()


def tail(n, cap, attn, tokens, rank, w_router, w_out, w_gate, w_up, w_down, chunks=8, depth=4):
    tok, hidden = tokens.shape
    width = hidden // chunks
    n_loc = rank.shape[0] // n
    vmem = pl.BlockSpec(memory_space=pltpu.VMEM)
    hbm = pl.BlockSpec(memory_space=pl.ANY)
    dma = pltpu.SemaphoreType.DMA
    weights = w_out.size + w_gate.size + w_up.size + w_down.size
    return pl.pallas_call(
        functools.partial(tail_body, n, cap),
        out_shape=(jax.ShapeDtypeStruct((tok, hidden), jnp.bfloat16),
                   jax.ShapeDtypeStruct((n_loc, n * cap, hidden), jnp.bfloat16)),
        in_specs=[vmem] * 4 + [hbm] * 4,
        out_specs=(vmem, hbm),
        scratch_shapes=[
            pltpu.VMEM((n, chunks, tok, width), jnp.bfloat16),
            pltpu.VMEM((tok, hidden), jnp.bfloat16),
            pltpu.VMEM((tok, hidden), jnp.bfloat16),
            pltpu.VMEM((depth, hidden, width), jnp.bfloat16),
            pltpu.VMEM((2, n_loc, cap, hidden), jnp.bfloat16),
            pltpu.VMEM((n, 2 * n_loc, tok), jnp.float32),
            pltpu.VMEM((n, 2 * n_loc, tok), jnp.float32),
            dma((depth,)), dma((2,)), dma((n,)), dma((n,)),
        ] + ring_scratch(n, chunks),
        cost_estimate=pl.CostEstimate(flops=2 * tok * weights, bytes_accessed=2 * weights, transcendentals=0),
        compiler_params=pltpu.CompilerParams(vmem_limit_bytes=44 * 2 ** 20, collective_id=0, has_side_effects=True),
        name='tail',
    )(attn, tokens, rank, w_router, w_out, w_gate, w_up, w_down)


def slot_ranks(expert_ids, n_experts):
    tok = expert_ids.shape[0]
    chosen = jnp.any(expert_ids[:, :, None] == jnp.arange(n_experts, dtype=jnp.int32), axis=1)
    earlier = jnp.tril(jnp.ones((tok, tok), jnp.bfloat16), -1)
    rank = jnp.dot(earlier, chosen.astype(jnp.bfloat16), preferred_element_type=jnp.float32)
    return jnp.where(chosen, rank, -1.0).T


def solution(mesh):
    row_spec = P(('dp', 'sp'), None)
    buf_spec = P(('dp', 'sp'), None, None)
    replicated = P()

    def local_step(tokens, w_query, w_key, w_value, w_out, w_gate, w_up, w_down, w_router, expert_ids):
        tok = tokens.shape[0]
        n_grp = mesh.shape['sp']
        n_experts = w_router.shape[1]
        cap = max(2, (tok * expert_ids.shape[1] // n_experts) * 2)
        me = lax.axis_index('sp').astype(jnp.int32).reshape(1)
        queries, kv_all = front(n_grp, tokens, w_key, w_value, w_query)
        attn = attention(me, queries, kv_all)
        rank = slot_ranks(expert_ids, n_experts)
        hidden_out, expert_buf = tail(n_grp, cap, attn, tokens, rank, w_router, w_out, w_gate, w_up, w_down)
        return hidden_out, expert_buf

    return jax.shard_map(local_step, mesh=mesh, in_specs=(row_spec,) + (replicated,) * 8 + (row_spec,), out_specs=(row_spec, buf_spec), check_vma=False)
```

```python
import functools
import math
import jax
import jax.numpy as jnp
from jax import lax
from jax.experimental import pallas as pl
from jax.experimental.pallas import tpu as pltpu
from jax.sharding import PartitionSpec as P

HEAD_DIM = 128
NT = (((1,), (1,)), ((), ()))
MESH = pl.DeviceIdType.MESH
LAG = 3


def attention_body(chunk, rows, me_ref, q_ref, k_ref, v_ref, o_ref, m_ref, l_ref, acc_ref, bias_ref):
    tok = q_ref.shape[0]
    heads = q_ref.shape[1] // HEAD_DIM
    per = rows // tok
    blocks = chunk // tok
    me = me_ref[0]
    factor = math.log2(math.e) / math.sqrt(HEAD_DIM)
    full = (me * tok) // chunk
    m_ref[...] = jnp.full(m_ref.shape, -jnp.inf, jnp.float32)
    l_ref[...] = jnp.zeros(l_ref.shape, jnp.float32)
    acc_ref[...] = jnp.zeros(acc_ref.shape, jnp.float32)
    pos = me * tok - full * chunk + lax.broadcasted_iota(jnp.int32, bias_ref.shape, 0)
    key = lax.broadcasted_iota(jnp.int32, bias_ref.shape, 1)
    bias_ref[...] = jnp.where(key <= pos, 0.0, -jnp.inf)

    groups = heads // per
    lanes = [slice(i * 128, (i + 1) * 128) for i in range(chunk // 128)]

    def step(c, masked):
        keys = k_ref[pl.ds(c * blocks, blocks), 0].reshape(chunk, HEAD_DIM)
        vals = v_ref[pl.ds(c * blocks, blocks), 0].reshape(chunk, HEAD_DIM)

        def score(g):
            q = jnp.concatenate([q_ref[:, (g * per + i) * HEAD_DIM:(g * per + i + 1) * HEAD_DIM] for i in range(per)], axis=0)
            return lax.dot_general(q, keys, NT, preferred_element_type=jnp.float32)

        ahead = score(0)
        for g in range(groups):
            s = ahead
            if g + 1 < groups:
                ahead = score(g + 1)
            s = [s[:, i] * factor for i in lanes]
            if masked:
                s = [(x.reshape(per, tok, 128) + bias_ref[:, i][None]).reshape(rows, 128) for x, i in zip(s, lanes)]
            sl = pl.ds(g * rows, rows)
            m_old = m_ref[sl, :]
            m_new = jnp.maximum(m_old, jnp.max(functools.reduce(jnp.maximum, s), axis=1, keepdims=True))
            p = [jnp.exp2(x - m_new) for x in s]
            alpha = jnp.exp2(m_old - m_new)
            l_ref[sl, :] = l_ref[sl, :] * alpha + functools.reduce(jnp.add, p)
            m_ref[sl, :] = m_new
            p = jnp.concatenate([x.astype(jnp.bfloat16) for x in p], axis=1)
            acc_ref[sl, :] = acc_ref[sl, :] * alpha + jnp.dot(p, vals, preferred_element_type=jnp.float32)

    @pl.loop(0, full)
    def _(c):
        step(c, False)

    step(full, True)
    for h in range(heads):
        sl = pl.ds(h * tok, tok)
        total = jnp.sum(l_ref[sl, :], axis=1, keepdims=True)
        o_ref[:, h * HEAD_DIM:(h + 1) * HEAD_DIM] = (acc_ref[sl, :] * (1.0 / total)).astype(o_ref.dtype)


def attention(me, queries, kv_all, chunk=512, rows=512):
    tok, width = queries.shape
    n_src, _, _, kv_width = kv_all.shape
    kv_heads = kv_width // HEAD_DIM
    cols = width // kv_heads
    all_rows = tok * cols // HEAD_DIM
    return pl.pallas_call(
        functools.partial(attention_body, chunk, rows),
        out_shape=pltpu.VMEM((tok, width), jnp.bfloat16),
        grid_spec=pltpu.PrefetchScalarGridSpec(
            num_scalar_prefetch=1,
            grid=(kv_heads,),
            in_specs=[
                pl.BlockSpec((tok, cols), lambda i, me: (0, i)),
                pl.BlockSpec((n_src, 1, tok, HEAD_DIM), lambda i, me: (0, 0, 0, i)),
                pl.BlockSpec((n_src, 1, tok, HEAD_DIM), lambda i, me: (0, 1, 0, i)),
            ],
            out_specs=pl.BlockSpec((tok, cols), lambda i, me: (0, i)),
            scratch_shapes=[
                pltpu.VMEM((all_rows, 128), jnp.float32),
                pltpu.VMEM((all_rows, 128), jnp.float32),
                pltpu.VMEM((all_rows, 128), jnp.float32),
                pltpu.VMEM((tok, chunk), jnp.float32),
            ],
        ),
        cost_estimate=pl.CostEstimate(flops=4 * tok * width * n_src * tok, bytes_accessed=4 * tok * width + 2 * kv_all.size, transcendentals=0),
        compiler_params=pltpu.CompilerParams(vmem_limit_bytes=36 * 2 ** 20),
        name='attention',
    )(me, queries, kv_all, kv_all)


class Ring:
    def __init__(self, n, buf, up_send, down_send, ring_recv, mate_send, mate_recv):
        self.n, self.len, self.chunks = n, n // 2, buf.shape[1]
        self.half = self.chunks // 2
        self.buf, self.up_send, self.down_send = buf, up_send, down_send
        self.ring_recv, self.mate_send, self.mate_recv = ring_recv, mate_send, mate_recv
        self.me = lax.axis_index('sp')
        self.mate = self.me + 1 - 2 * lax.rem(self.me, 2)
        self.up = lax.rem(self.me + 2, n)
        self.down = lax.rem(self.me + n - 2, n)

    def barrier(self):
        sem = pltpu.get_barrier_semaphore()
        for i in range(1, self.n):
            pl.semaphore_signal(sem, inc=1, device_id={'sp': lax.rem(self.me + i, self.n)}, device_id_type=MESH)
        pl.semaphore_wait(sem, self.n - 1)

    def owner(self, delta, base=None):
        return lax.rem((self.me if base is None else base) + 2 * delta, self.n)

    def copy(self, delta, j, send_sem, recv_sem, target):
        piece = self.buf.at[self.owner(delta), j]
        return pltpu.make_async_remote_copy(src_ref=piece, dst_ref=piece, send_sem=send_sem, recv_sem=recv_sem,
                                            device_id={'sp': target}, device_id_type=MESH)

    def up_copy(self, dist, j):
        delta = lax.rem(self.len - dist, self.len)
        return self.copy(delta, j, self.up_send.at[dist, j], self.ring_recv.at[lax.rem(delta + self.len - 1, self.len), j], self.up)

    def down_copy(self, dist, j):
        return self.copy(dist, j, self.down_send.at[dist, j], self.ring_recv.at[dist + 1, j], self.down)

    def mate_copy(self, delta, j):
        return self.copy(delta, j, self.mate_send.at[delta, j], self.mate_recv.at[delta, j], self.mate)

    def wait_ring(self, delta, j):
        self.copy(delta, j, self.mate_send.at[delta, j], self.ring_recv.at[delta, j], self.mate).wait_recv()

    def wait_mate(self, delta, j):
        piece = self.buf.at[self.owner(delta, self.mate), j]
        pltpu.make_async_remote_copy(src_ref=piece, dst_ref=piece, send_sem=self.mate_send.at[delta, j], recv_sem=self.mate_recv.at[delta, j],
                                     device_id={'sp': self.mate}, device_id_type=MESH).wait_recv()

    def send_own(self, j):
        self.up_copy(0, j).start()
        self.down_copy(0, j).start()
        self.mate_copy(0, j).start()

    def step(self, r):
        dist, j = r // self.chunks + 1, lax.rem(r, self.chunks)
        last = 2 * self.chunks
        self.wait_ring(self.len - dist, j)

        @pl.when(r < last + self.half)
        def _():
            self.up_copy(dist, j).start()

        self.mate_copy(self.len - dist, j).start()
        self.wait_ring(dist, j)

        @pl.when((r < last) | (r >= last + self.half))
        def _():
            self.down_copy(dist, j).start()

        self.mate_copy(dist, j).start()

    def far_step(self, i):
        far = self.len // 2
        for j in (i, i + self.half):
            self.wait_ring(far, j)
            self.mate_copy(far, j).start()

    def drain(self):
        far = self.len // 2

        @pl.loop(0, self.chunks)
        def _(j):
            for dist in range(far):
                @pl.when((dist < far - 1) | (j < self.half))
                def _(dist=dist):
                    self.up_copy(dist, j).wait_send()

                @pl.when((dist < far - 1) | (j >= self.half))
                def _(dist=dist):
                    self.down_copy(dist, j).wait_send()
            for delta in range(self.len):
                self.mate_copy(delta, j).wait_send()


def ring_scratch(n, chunks):
    length, far = n // 2, n // 4
    dma = pltpu.SemaphoreType.DMA
    return [dma((far, chunks)), dma((far, chunks)), dma((length, chunks)), dma((length, chunks)), dma((length, chunks))]


class Tiles:
    def __init__(self, slots, sems, groups):
        self.slots, self.sems, self.groups = slots, sems, groups
        self.depth, self.total = slots.shape[0], groups[-1][0]

    def copy(self, tile, slot):
        return pltpu.make_async_copy(tile, self.slots.at[slot], self.sems.at[slot])

    def start(self, t):
        first = 0
        for end, pick in self.groups:
            @pl.when((t >= first) & (t < end))
            def _(first=first, pick=pick):
                for cond, tile in pick(t - first):
                    if cond is None:
                        self.copy(tile, lax.rem(t, self.depth)).start()
                    else:
                        @pl.when(cond)
                        def _(tile=tile):
                            self.copy(tile, lax.rem(t, self.depth)).start()
            first = end

    def prime(self):
        for t in range(self.depth - 1):
            self.start(jnp.int32(t))

    def take(self, t):
        self.start(t + self.depth - 1)
        slot = lax.rem(t, self.depth)
        self.copy(self.groups[0][1](0)[0][1], slot).wait()
        return self.slots.at[slot]


def columns(j, width):
    return pl.ds(pl.multiple_of(j * width, width), width)


def front_body(n, x_ref, wk_ref, wv_ref, wq_ref, q_ref, kv_ref, buf, slots, sems, out_sem, *ring_sems):
    ring = Ring(n, buf, *ring_sems)
    width = slots.shape[2]
    count = wq_ref.shape[1] // width
    tiles = Tiles(slots, sems, (
        (1, lambda t: [(None, wk_ref)]),
        (2, lambda t: [(None, wv_ref)]),
        (2 + count, lambda t: [(None, wq_ref.at[:, columns(t, width)])]),
    ))
    tiles.prime()
    ring.barrier()
    for c in range(2):
        buf[ring.me, c] = jnp.dot(x_ref[...], tiles.take(jnp.int32(c))[...], preferred_element_type=jnp.float32).astype(jnp.bfloat16)
        ring.send_own(jnp.int32(c))

    steps = 3 * ring.chunks

    @pl.loop(0, count)
    def _(j):
        q_ref[:, columns(j, width)] = jnp.dot(x_ref[...], tiles.take(j + 2)[...], preferred_element_type=jnp.float32).astype(jnp.bfloat16)

        @pl.when((lax.rem(j, 2) == 1) & (j >= 3) & (j < 3 + 2 * steps))
        def _():
            ring.step((j - 3) // 2)

    for r in range(max(0, (count - 2) // 2), steps):
        ring.step(jnp.int32(r))
    ring.far_step(jnp.int32(0))
    for delta in range(ring.len):
        for c in range(2):
            ring.wait_mate(delta, c)
    out = pltpu.make_async_copy(buf, kv_ref, out_sem.at[0])
    out.start()
    ring.drain()
    out.wait()


def front(n, tokens, w_key, w_value, w_query, depth=4):
    tok, hidden = tokens.shape
    width = w_key.shape[1]
    vmem = pl.BlockSpec(memory_space=pltpu.VMEM)
    hbm = pl.BlockSpec(memory_space=pltpu.HBM)
    dma = pltpu.SemaphoreType.DMA
    weights = w_key.size + w_value.size + w_query.size
    return pl.pallas_call(
        functools.partial(front_body, n),
        out_shape=(pltpu.VMEM((tok, w_query.shape[1]), jnp.bfloat16),
                   pltpu.VMEM((n, 2, tok, width), jnp.bfloat16)),
        in_specs=[vmem] + [hbm] * 3,
        out_specs=(vmem, vmem),
        scratch_shapes=[
            pltpu.VMEM((n, 2, tok, width), jnp.bfloat16),
            pltpu.VMEM((depth, hidden, width), jnp.bfloat16),
            dma((depth,)), dma((1,)),
        ] + ring_scratch(n, 2),
        cost_estimate=pl.CostEstimate(flops=2 * tok * weights, bytes_accessed=2 * weights, transcendentals=0),
        compiler_params=pltpu.CompilerParams(vmem_limit_bytes=52 * 2 ** 20, collective_id=1, has_side_effects=True),
        name='front',
    )(tokens, w_key, w_value, w_query)


def tail_body(n, cap, o_ref, x_ref, ids_ref, router_ref, wo_ref, wg_ref, wu_ref, wd_ref, y_ref, e_ref,
              buf, row_ref, act_ref, slots, table_out, table_in, sems, table_send, table_recv, *ring_sems):
    f32, bf16 = jnp.float32, jnp.bfloat16
    ring = Ring(n, buf, *ring_sems)
    me = ring.me
    chunks, tok, width = buf.shape[1:]
    depth = slots.shape[1]
    parts = o_ref.shape[1] // depth
    n_exp = router_ref.shape[1]
    n_loc = n_exp // n
    tiles = Tiles(slots, sems, (
        (parts * chunks, lambda t: [(None, wo_ref.at[columns(lax.rem(t, parts), depth), columns(t // parts, width)])]),
        ((parts + 2) * chunks, lambda t: [(lax.rem(t, 2) == 0, wg_ref.at[:, columns(t // 2, width)]),
                                          (lax.rem(t, 2) == 1, wu_ref.at[:, columns(t // 2, width)])]),
        ((parts + 3) * chunks, lambda t: [(None, wd_ref.at[:, columns(t, width)])]),
    ))
    tiles.prime()
    ring.barrier()

    @pl.loop(0, chunks)
    def _(j):
        acc = x_ref[:, columns(j, width)].astype(f32)
        part = None
        for i in range(parts):
            prod = jnp.dot(o_ref[:, i * depth:(i + 1) * depth], tiles.take(parts * j + i)[...], preferred_element_type=f32)
            part = prod if part is None else part + prod
        h = (acc + part).astype(bf16)
        buf[me, j] = h
        row_ref[:, columns(j, width)] = h
        ring.send_own(j)

        @pl.when(j >= LAG)
        def _():
            ring.step(j - LAG)

    expert = lax.broadcasted_iota(jnp.int32, (n_exp, tok), 0)
    chosen = functools.reduce(jnp.logical_or, [ids_ref[c:c + 1, :] == expert for c in range(ids_ref.shape[0])])
    earlier = lax.broadcasted_iota(jnp.int32, (tok, tok), 0) < lax.broadcasted_iota(jnp.int32, (tok, tok), 1)
    count = jnp.dot(jnp.where(chosen, 1.0, 0.0).astype(bf16), jnp.where(earlier, 1.0, 0.0).astype(bf16), preferred_element_type=f32)
    rank = jnp.where(chosen, count, -1.0)
    gate = jax.nn.sigmoid(jnp.dot(row_ref[...], router_ref[...], preferred_element_type=f32)).T
    for d in range(n):
        table_out[d, :n_loc] = rank[d * n_loc:(d + 1) * n_loc]
        table_out[d, n_loc:] = gate[d * n_loc:(d + 1) * n_loc]
    table_in[me] = table_out[me]

    def table_copy(i):
        dst = lax.rem(me + i, n)
        return pltpu.make_async_remote_copy(src_ref=table_out.at[dst], dst_ref=table_in.at[me], send_sem=table_send.at[i], recv_sem=table_recv.at[i],
                                            device_id={'sp': dst}, device_id_type=MESH)

    def table_arrival(i):
        src = lax.rem(me + n - i, n)
        return pltpu.make_async_remote_copy(src_ref=table_out.at[src], dst_ref=table_in.at[src], send_sem=table_send.at[i], recv_sem=table_recv.at[i],
                                            device_id={'sp': src}, device_id_type=MESH)

    for i in range(1, n):
        table_copy(i).start()

    base = parts * chunks

    @pl.loop(0, chunks)
    def _(j):
        h = row_ref[...]
        g = jnp.dot(h, tiles.take(base + 2 * j)[...], preferred_element_type=f32)
        u = jnp.dot(h, tiles.take(base + 2 * j + 1)[...], preferred_element_type=f32)
        act_ref[:, columns(j, width)] = (g * jax.nn.sigmoid(g) * u).astype(bf16)
        ring.step(j + chunks - LAG)

    base += 2 * chunks

    @pl.loop(0, chunks)
    def _(j):
        y = jnp.dot(act_ref[...], tiles.take(base + j)[...], preferred_element_type=f32)
        y_ref[:, columns(j, width)] = (row_ref[:, columns(j, width)].astype(f32) + y).astype(bf16)

        @pl.when(lax.rem(j, 2) == 1)
        def _():
            ring.step(2 * chunks - LAG + j // 2)

    for i in range(1, n):
        table_arrival(i).wait_recv()

    def expand(src, js):
        shape = (n_loc, cap, tok)
        table = table_in[src]
        place = lax.broadcasted_iota(jnp.int32, shape, 1).astype(f32)
        sel = jnp.where(jnp.broadcast_to(table[:n_loc][:, None, :], shape) == place, 1.0, 0.0)
        scale = jnp.sum(sel * jnp.broadcast_to(table[n_loc:][:, None, :], shape), axis=2, keepdims=True).reshape(n_loc * cap, 1)
        sel = sel.reshape(n_loc * cap, tok).astype(bf16)
        for j in js:
            rows = jnp.dot(sel, buf[src, j], preferred_element_type=f32) * scale
            e_ref[:, pl.ds(pl.multiple_of(src * cap, cap), cap), columns(j, width)] = rows.astype(bf16).reshape(n_loc, cap, width)

    def expand_pair(delta):
        expand(ring.owner(delta), range(chunks))

        @pl.loop(0, chunks)
        def _(j):
            ring.wait_mate(delta, j)

        expand(ring.owner(delta, ring.mate), range(chunks))

    done = 2 * chunks - LAG + chunks // 2
    length, far = n // 2, n // 4
    near = 2 * far - 3

    @pl.loop(0, 3 * chunks - done)
    def _(k):
        ring.step(done + k)

        @pl.when(k < near)
        def _():
            expand_pair(jnp.where(lax.rem(k, 2) == 1, length - (k + 1) // 2, k // 2))

    def expand_far(i):
        js = (i, i + chunks // 2)
        expand(ring.owner(far), js)
        for j in js:
            ring.wait_mate(far, j)
        expand(ring.owner(far, ring.mate), js)

    half = chunks // 2
    for i in range(half):
        ring.far_step(jnp.int32(i))
        if i < 2:
            expand_pair(jnp.int32(far + 1 - 2 * i))

    @pl.loop(0, half)
    def _(i):
        expand_far(i)

    ring.drain()
    for i in range(1, n):
        table_copy(i).wait_send()


def tail(n, cap, attn, tokens, ids, w_router, w_out, w_gate, w_up, w_down, chunks=8, depth=3):
    tok, hidden = tokens.shape
    width = hidden // chunks
    n_loc = w_router.shape[1] // n
    vmem = pl.BlockSpec(memory_space=pltpu.VMEM)
    hbm = pl.BlockSpec(memory_space=pltpu.HBM)
    dma = pltpu.SemaphoreType.DMA
    weights = w_out.size + w_gate.size + w_up.size + w_down.size
    return pl.pallas_call(
        functools.partial(tail_body, n, cap),
        out_shape=(pltpu.VMEM((tok, hidden), jnp.bfloat16),
                   pltpu.VMEM((n_loc, n * cap, hidden), jnp.bfloat16)),
        in_specs=[vmem] * 4 + [hbm] * 4,
        out_specs=(vmem, vmem),
        scratch_shapes=[
            pltpu.VMEM((n, chunks, tok, width), jnp.bfloat16),
            pltpu.VMEM((tok, hidden), jnp.bfloat16),
            pltpu.VMEM((tok, hidden), jnp.bfloat16),
            pltpu.VMEM((depth, hidden, width), jnp.bfloat16),
            pltpu.VMEM((n, 2 * n_loc, tok), jnp.float32),
            pltpu.VMEM((n, 2 * n_loc, tok), jnp.float32),
            dma((depth,)), dma((n,)), dma((n,)),
        ] + ring_scratch(n, chunks),
        cost_estimate=pl.CostEstimate(flops=2 * tok * weights, bytes_accessed=2 * weights, transcendentals=0),
        compiler_params=pltpu.CompilerParams(vmem_limit_bytes=41 * 2 ** 20, collective_id=0, has_side_effects=True),
        name='tail',
    )(attn, tokens, ids, w_router, w_out, w_gate, w_up, w_down)


def solution(mesh):
    row_spec = P(('dp', 'sp'), None)
    buf_spec = P(('dp', 'sp'), None, None)
    replicated = P()

    def local_step(tokens, w_query, w_key, w_value, w_out, w_gate, w_up, w_down, w_router, expert_ids):
        tok = tokens.shape[0]
        n_grp = mesh.shape['sp']
        n_experts = w_router.shape[1]
        cap = max(2, (tok * expert_ids.shape[1] // n_experts) * 2)
        me = lax.axis_index('sp').astype(jnp.int32).reshape(1)
        queries, kv_all = front(n_grp, tokens, w_key, w_value, w_query)
        attn = pltpu.with_memory_space_constraint(attention(me, queries, kv_all), pltpu.VMEM)
        hidden_out, expert_buf = tail(n_grp, cap, attn, tokens, expert_ids.T, w_router, w_out, w_gate, w_up, w_down)
        return hidden_out, expert_buf

    return jax.shard_map(local_step, mesh=mesh, in_specs=(row_spec,) + (replicated,) * 8 + (row_spec,), out_specs=(row_spec, buf_spec), check_vma=False)
```

```python
import functools
import math
import jax
import jax.numpy as jnp
from jax import lax
from jax.experimental import pallas as pl
from jax.experimental.pallas import tpu as pltpu
from jax.sharding import PartitionSpec as P

HEAD_DIM = 128
NT = (((1,), (1,)), ((), ()))
MESH = pl.DeviceIdType.MESH


class Ring:
    def __init__(self, n, piece, up_send, down_send, ring_recv, mate_send, mate_recv):
        self.n, self.len, self.chunks = n, n // 2, up_send.shape[1]
        self.half = self.chunks // 2
        self.piece, self.up_send, self.down_send = piece, up_send, down_send
        self.ring_recv, self.mate_send, self.mate_recv = ring_recv, mate_send, mate_recv
        self.me = lax.axis_index('sp')
        self.mate = self.me + 1 - 2 * lax.rem(self.me, 2)
        self.up = lax.rem(self.me + 2, n)
        self.down = lax.rem(self.me + n - 2, n)

    def barrier(self):
        sem = pltpu.get_barrier_semaphore()
        for i in range(1, self.n):
            pl.semaphore_signal(sem, inc=1, device_id={'sp': lax.rem(self.me + i, self.n)}, device_id_type=MESH)
        pl.semaphore_wait(sem, self.n - 1)

    def owner(self, delta, base=None):
        return lax.rem((self.me if base is None else base) + 2 * delta, self.n)

    def copy(self, delta, j, send_sem, recv_sem, target):
        piece = self.piece(self.owner(delta), j)
        return pltpu.make_async_remote_copy(src_ref=piece, dst_ref=piece, send_sem=send_sem, recv_sem=recv_sem,
                                            device_id={'sp': target}, device_id_type=MESH)

    def up_copy(self, dist, j):
        delta = lax.rem(self.len - dist, self.len)
        return self.copy(delta, j, self.up_send.at[dist, j], self.ring_recv.at[lax.rem(delta + self.len - 1, self.len), j], self.up)

    def down_copy(self, dist, j):
        return self.copy(dist, j, self.down_send.at[dist, j], self.ring_recv.at[dist + 1, j], self.down)

    def mate_copy(self, delta, j):
        return self.copy(delta, j, self.mate_send.at[delta, j], self.mate_recv.at[delta, j], self.mate)

    def wait_ring(self, delta, j):
        self.copy(delta, j, self.mate_send.at[delta, j], self.ring_recv.at[delta, j], self.mate).wait_recv()

    def wait_mate(self, delta, j):
        piece = self.piece(self.owner(delta, self.mate), j)
        pltpu.make_async_remote_copy(src_ref=piece, dst_ref=piece, send_sem=self.mate_send.at[delta, j], recv_sem=self.mate_recv.at[delta, j],
                                     device_id={'sp': self.mate}, device_id_type=MESH).wait_recv()

    def send_own(self, j):
        self.up_copy(0, j).start()
        self.down_copy(0, j).start()
        self.mate_copy(0, j).start()

    def step(self, r):
        dist, j = r // self.chunks + 1, lax.rem(r, self.chunks)
        last = 2 * self.chunks
        self.wait_ring(self.len - dist, j)

        @pl.when(r < last + self.half)
        def _():
            self.up_copy(dist, j).start()

        self.mate_copy(self.len - dist, j).start()
        self.wait_ring(dist, j)

        @pl.when((r < last) | (r >= last + self.half))
        def _():
            self.down_copy(dist, j).start()

        self.mate_copy(dist, j).start()

    def far_step(self, i):
        far = self.len // 2
        for j in (i, i + self.half):
            self.wait_ring(far, j)
            self.mate_copy(far, j).start()

    def drain(self):
        far = self.len // 2

        @pl.loop(0, self.chunks)
        def _(j):
            for dist in range(far):
                @pl.when((dist < far - 1) | (j < self.half))
                def _(dist=dist):
                    self.up_copy(dist, j).wait_send()

                @pl.when((dist < far - 1) | (j >= self.half))
                def _(dist=dist):
                    self.down_copy(dist, j).wait_send()
            for delta in range(self.len):
                self.mate_copy(delta, j).wait_send()


def ring_scratch(n, chunks):
    length, far = n // 2, n // 4
    dma = pltpu.SemaphoreType.DMA
    return [dma((far, chunks)), dma((far, chunks)), dma((length, chunks)), dma((length, chunks)), dma((length, chunks))]


class Tiles:
    def __init__(self, slots, sems, groups):
        self.slots, self.sems, self.groups = slots, sems, groups
        self.depth, self.total = slots.shape[0], groups[-1][0]

    def copy(self, tile, slot):
        return pltpu.make_async_copy(tile, self.slots.at[slot], self.sems.at[slot])

    def start(self, t):
        first = 0
        for end, pick in self.groups:
            @pl.when((t >= first) & (t < end))
            def _(first=first, pick=pick):
                for cond, tile in pick(t - first):
                    if cond is None:
                        self.copy(tile, lax.rem(t, self.depth)).start()
                    else:
                        @pl.when(cond)
                        def _(tile=tile):
                            self.copy(tile, lax.rem(t, self.depth)).start()
            first = end

    def prime(self):
        for t in range(self.depth - 1):
            self.start(jnp.int32(t))

    def take(self, t):
        self.start(t + self.depth - 1)
        slot = lax.rem(t, self.depth)
        self.copy(self.groups[0][1](0)[0][1], slot).wait()
        return self.slots.at[slot]


def columns(j, width):
    return pl.ds(pl.multiple_of(j * width, width), width)


def block_body(n, cap, span, rows, x_ref, ids_ref, wk_ref, wv_ref, wq_ref, wr_ref, wo_ref, wg_ref, wu_ref, wd_ref, y_ref, e_ref,
               buf, q_ref, row_ref, slots, router_ref, m_ref, l_ref, acc_ref, bias_ref, table_out, table_in,
               sems, router_sem, table_send, table_recv, *ring_sems):
    f32, bf16 = jnp.float32, jnp.bfloat16
    chunks, tok, width = buf.shape[1:]
    depth = slots.shape[1]
    n_exp = router_ref.shape[1]
    n_loc = n_exp // n
    kv_heads = width // HEAD_DIM
    q_tiles = q_ref.shape[1] // width
    parts = q_ref.shape[1] // depth
    act_ref = q_ref.at[:, :depth]

    def kv_piece(src, j):
        return e_ref.at[lax.rem(src, n_loc), columns(src // n_loc, tok), columns(j, width)]

    kv_ring = Ring(n, kv_piece, *ring_sems[:5])
    ring = Ring(n, lambda src, j: buf.at[src, j], *ring_sems[5:])
    me = ring.me
    ends = [1, 2, 2 + q_tiles, 2 + q_tiles + parts * chunks, 2 + q_tiles + (parts + 2) * chunks, 2 + q_tiles + (parts + 3) * chunks]
    tiles = Tiles(slots, sems, (
        (ends[0], lambda t: [(None, wk_ref)]),
        (ends[1], lambda t: [(None, wv_ref)]),
        (ends[2], lambda t: [(None, wq_ref.at[:, columns(t, width)])]),
        (ends[3], lambda t: [(None, wo_ref.at[columns(lax.rem(t, parts), depth), columns(t // parts, width)])]),
        (ends[4], lambda t: [(lax.rem(t, 2) == 0, wg_ref.at[:, columns(t // 2, width)]),
                             (lax.rem(t, 2) == 1, wu_ref.at[:, columns(t // 2, width)])]),
        (ends[5], lambda t: [(None, wd_ref.at[:, columns(t, width)])]),
    ))
    tiles.prime()
    router_copy = pltpu.make_async_copy(wr_ref, router_ref, router_sem.at[0])
    router_copy.start()
    ring.barrier()

    for c in range(2):
        part = jnp.dot(x_ref[...], tiles.take(jnp.int32(c))[...], preferred_element_type=f32).astype(bf16)
        e_ref[lax.rem(me, n_loc), columns(me // n_loc, tok), c * width:(c + 1) * width] = part
        kv_ring.send_own(jnp.int32(c))

    kv_steps = 3 * kv_ring.chunks

    @pl.loop(0, q_tiles)
    def _(j):
        q_ref[:, columns(j, width)] = jnp.dot(x_ref[...], tiles.take(j + 2)[...], preferred_element_type=f32).astype(bf16)

        @pl.when((lax.rem(j, 2) == 1) & (j >= 3) & (j < 3 + 2 * kv_steps))
        def _():
            kv_ring.step((j - 3) // 2)

    for r in range((q_tiles - 2) // 2, kv_steps):
        kv_ring.step(jnp.int32(r))
    kv_ring.far_step(jnp.int32(0))
    for delta in range(kv_ring.len):
        for c in range(2):
            kv_ring.wait_mate(delta, c)

    per = rows // tok
    heads = q_ref.shape[1] // (kv_heads * HEAD_DIM)
    groups = heads // per
    blocks = span // tok
    halves = n_loc // blocks
    factor = math.log2(math.e) / math.sqrt(HEAD_DIM)
    full = (me * tok) // span
    lanes = [slice(i * 128, (i + 1) * 128) for i in range(span // 128)]
    pos = me * tok - full * span + lax.broadcasted_iota(jnp.int32, bias_ref.shape, 0)
    bias_ref[...] = jnp.where(lax.broadcasted_iota(jnp.int32, bias_ref.shape, 1) <= pos, 0.0, -jnp.inf)

    def head_columns(i, h):
        return columns(i * heads + h, HEAD_DIM)

    def key_block(c, col):
        return e_ref[pl.ds(lax.rem(c, halves) * blocks, blocks), columns(c // halves, tok), columns(col, HEAD_DIM)].reshape(span, HEAD_DIM)

    def attend(i, c, first):
        keys = key_block(c, i)
        vals = key_block(c, kv_heads + i)

        def score(g):
            q = jnp.concatenate([q_ref[:, head_columns(i, g * per + h)] for h in range(per)], axis=0)
            return lax.dot_general(q, keys, NT, preferred_element_type=f32)

        ahead = score(0)
        for g in range(groups):
            s = ahead
            if g + 1 < groups:
                ahead = score(g + 1)
            s = [s[:, k] * factor for k in lanes]
            sl = pl.ds(g * rows, rows)
            if first:
                s = [(x.reshape(per, tok, 128) + bias_ref[:, k][None]).reshape(rows, 128) for x, k in zip(s, lanes)]
            m_new = jnp.max(functools.reduce(jnp.maximum, s), axis=1, keepdims=True)
            if first:
                m_new = jnp.broadcast_to(m_new, (rows, 128))
            else:
                m_old = m_ref[sl, :]
                m_new = jnp.maximum(m_old, m_new)
                alpha = jnp.exp2(m_old - m_new)
            m_ref[sl, :] = m_new
            p = [jnp.exp2(x - m_new) for x in s]
            total = functools.reduce(jnp.add, p)
            out = jnp.dot(jnp.concatenate([x.astype(bf16) for x in p], axis=1), vals, preferred_element_type=f32)
            l_ref[sl, :] = total if first else l_ref[sl, :] * alpha + total
            acc_ref[sl, :] = out if first else acc_ref[sl, :] * alpha + out

    @pl.loop(0, kv_heads)
    def _(i):
        attend(i, full, True)

        @pl.loop(0, full)
        def _(c):
            attend(i, c, False)

        for h in range(heads):
            sl = pl.ds(h * tok, tok)
            total = jnp.sum(l_ref[sl, :], axis=1, keepdims=True)
            q_ref[:, head_columns(i, h)] = (acc_ref[sl, :] * (1.0 / total)).astype(bf16)

    @pl.loop(0, chunks)
    def _(j):
        part = None
        for i in range(parts):
            prod = jnp.dot(q_ref[:, i * depth:(i + 1) * depth], tiles.take(ends[2] + parts * j + i)[...], preferred_element_type=f32)
            part = prod if part is None else part + prod
        h = (x_ref[:, columns(j, width)].astype(f32) + part).astype(bf16)
        buf[me, j] = h
        row_ref[:, columns(j, width)] = h
        ring.send_own(j)

    router_copy.wait()
    expert = lax.broadcasted_iota(jnp.int32, (n_exp, tok), 0)
    chosen = functools.reduce(jnp.logical_or, [ids_ref[c:c + 1, :] == expert for c in range(ids_ref.shape[0])])
    earlier = lax.broadcasted_iota(jnp.int32, (tok, tok), 0) < lax.broadcasted_iota(jnp.int32, (tok, tok), 1)
    count = jnp.dot(jnp.where(chosen, 1.0, 0.0).astype(bf16), jnp.where(earlier, 1.0, 0.0).astype(bf16), preferred_element_type=f32)
    rank = jnp.where(chosen, count, -1.0)
    gate = jax.nn.sigmoid(jnp.dot(row_ref[...], router_ref[...], preferred_element_type=f32)).T
    for d in range(n):
        table_out[d, :n_loc] = rank[d * n_loc:(d + 1) * n_loc]
        table_out[d, n_loc:] = gate[d * n_loc:(d + 1) * n_loc]
    table_in[me] = table_out[me]

    def table_copy(i):
        dst = lax.rem(me + i, n)
        return pltpu.make_async_remote_copy(src_ref=table_out.at[dst], dst_ref=table_in.at[me], send_sem=table_send.at[i], recv_sem=table_recv.at[i],
                                            device_id={'sp': dst}, device_id_type=MESH)

    def table_arrival(i):
        src = lax.rem(me + n - i, n)
        return pltpu.make_async_remote_copy(src_ref=table_out.at[src], dst_ref=table_in.at[src], send_sem=table_send.at[i], recv_sem=table_recv.at[i],
                                            device_id={'sp': src}, device_id_type=MESH)

    for i in range(1, n):
        table_copy(i).start()

    half = chunks // 2

    @pl.loop(0, chunks)
    def _(j):
        h = row_ref[...]
        g = jnp.dot(h, tiles.take(ends[3] + 2 * j)[...], preferred_element_type=f32)
        u = jnp.dot(h, tiles.take(ends[3] + 2 * j + 1)[...], preferred_element_type=f32)
        act_ref[:, columns(j, width)] = (g * jax.nn.sigmoid(g) * u).astype(bf16)
        ring.step(j + jnp.minimum(j, half))

        @pl.when(j < half)
        def _():
            ring.step(2 * j + 1)

    @pl.loop(0, chunks)
    def _(j):
        y = jnp.dot(act_ref[...], tiles.take(ends[4] + j)[...], preferred_element_type=f32)
        y_ref[:, columns(j, width)] = (row_ref[:, columns(j, width)].astype(f32) + y).astype(bf16)

        @pl.when(lax.rem(j, 2) == 1)
        def _():
            ring.step(chunks + half + j // 2)

    kv_ring.drain()
    for i in range(1, n):
        table_arrival(i).wait_recv()

    def expand(src, js):
        shape = (n_loc, cap, tok)
        table = table_in[src]
        place = lax.broadcasted_iota(jnp.int32, shape, 1).astype(f32)
        sel = jnp.where(jnp.broadcast_to(table[:n_loc][:, None, :], shape) == place, 1.0, 0.0)
        scale = jnp.sum(sel * jnp.broadcast_to(table[n_loc:][:, None, :], shape), axis=2, keepdims=True).reshape(n_loc * cap, 1)
        sel = sel.reshape(n_loc * cap, tok).astype(bf16)
        for j in js:
            out = jnp.dot(sel, buf[src, j], preferred_element_type=f32) * scale
            e_ref[:, pl.ds(pl.multiple_of(src * cap, cap), cap), columns(j, width)] = out.astype(bf16).reshape(n_loc, cap, width)

    def expand_pair(delta):
        expand(ring.owner(delta), range(chunks))

        @pl.loop(0, chunks)
        def _(j):
            ring.wait_mate(delta, j)

        expand(ring.owner(delta, ring.mate), range(chunks))

    length, far = n // 2, n // 4
    near = 2 * far - 3

    @pl.loop(0, chunks)
    def _(k):
        ring.step(2 * chunks + k)

        @pl.when(k < near)
        def _():
            expand_pair(jnp.where(lax.rem(k, 2) == 1, length - (k + 1) // 2, k // 2))

    def expand_far(i):
        js = (i, i + half)
        expand(ring.owner(far), js)
        for j in js:
            ring.wait_mate(far, j)
        expand(ring.owner(far, ring.mate), js)

    @pl.loop(0, half)
    def _(i):
        ring.far_step(i)

        @pl.when(i < 2)
        def _():
            expand_pair(far + 1 - 2 * i)

        @pl.when(i > 0)
        def _():
            expand_far(i - 1)

    expand_far(jnp.int32(half - 1))
    ring.drain()
    for i in range(1, n):
        table_copy(i).wait_send()


def moe_block(n, cap, tokens, ids, w_key, w_value, w_query, w_router, w_out, w_gate, w_up, w_down, depth=3, span=512, rows=512):
    tok, hidden = tokens.shape
    width = w_key.shape[1]
    q_width = w_query.shape[1]
    chunks = hidden // width
    n_exp = w_router.shape[1]
    n_loc = n_exp // n
    all_rows = tok * q_width // width
    vmem = pl.BlockSpec(memory_space=pltpu.VMEM)
    hbm = pl.BlockSpec(memory_space=pltpu.HBM)
    dma = pltpu.SemaphoreType.DMA
    weights = 2 * w_key.size + w_query.size + w_out.size + w_gate.size + w_up.size + w_down.size
    return pl.pallas_call(
        functools.partial(block_body, n, cap, span, rows),
        out_shape=(pltpu.VMEM((tok, hidden), jnp.bfloat16), pltpu.VMEM((n_loc, n * cap, hidden), jnp.bfloat16)),
        in_specs=[vmem] * 2 + [hbm] * 8,
        out_specs=(vmem, vmem),
        scratch_shapes=[
            pltpu.VMEM((n, chunks, tok, width), jnp.bfloat16),
            pltpu.VMEM((tok, q_width), jnp.bfloat16),
            pltpu.VMEM((tok, hidden), jnp.bfloat16),
            pltpu.VMEM((depth, hidden, width), jnp.bfloat16),
            pltpu.VMEM(w_router.shape, jnp.bfloat16),
            pltpu.VMEM((all_rows, 128), jnp.float32),
            pltpu.VMEM((all_rows, 128), jnp.float32),
            pltpu.VMEM((all_rows, 128), jnp.float32),
            pltpu.VMEM((tok, span), jnp.float32),
            pltpu.VMEM((n, 2 * n_loc, tok), jnp.float32),
            pltpu.VMEM((n, 2 * n_loc, tok), jnp.float32),
            dma((depth,)), dma((1,)), dma((n,)), dma((n,)),
        ] + ring_scratch(n, 2) + ring_scratch(n, chunks),
        cost_estimate=pl.CostEstimate(flops=2 * tok * weights, bytes_accessed=2 * weights, transcendentals=0),
        compiler_params=pltpu.CompilerParams(vmem_limit_bytes=45 * 2 ** 20, collective_id=0, has_side_effects=True),
        name='moe_block',
    )(tokens, ids, w_key, w_value, w_query, w_router, w_out, w_gate, w_up, w_down)


def solution(mesh):
    row_spec = P(('dp', 'sp'), None)
    buf_spec = P(('dp', 'sp'), None, None)
    replicated = P()

    def local_step(tokens, w_query, w_key, w_value, w_out, w_gate, w_up, w_down, w_router, expert_ids):
        tok = tokens.shape[0]
        n_grp = mesh.shape['sp']
        n_experts = w_router.shape[1]
        cap = max(2, (tok * expert_ids.shape[1] // n_experts) * 2)
        hidden_out, expert_buf = moe_block(n_grp, cap, tokens, expert_ids.T, w_key, w_value, w_query, w_router, w_out, w_gate, w_up, w_down)
        return hidden_out, expert_buf

    return jax.shard_map(local_step, mesh=mesh, in_specs=(row_spec,) + (replicated,) * 8 + (row_spec,), out_specs=(row_spec, buf_spec), check_vma=False)
```

```python
import functools
import math
import jax
import jax.numpy as jnp
from jax import lax
from jax.experimental import pallas as pl
from jax.experimental.pallas import tpu as pltpu
from jax.sharding import PartitionSpec as P

HEAD_DIM = 128
NT = (((1,), (1,)), ((), ()))
MESH = pl.DeviceIdType.MESH


class Ring:
    def __init__(self, n, piece, up_send, down_send, ring_recv, mate_send, mate_recv):
        self.n, self.len, self.chunks = n, n // 2, up_send.shape[1]
        self.half = self.chunks // 2
        self.piece, self.up_send, self.down_send = piece, up_send, down_send
        self.ring_recv, self.mate_send, self.mate_recv = ring_recv, mate_send, mate_recv
        self.me = lax.axis_index('sp')
        self.mate = self.me + 1 - 2 * lax.rem(self.me, 2)
        self.up = lax.rem(self.me + 2, n)
        self.down = lax.rem(self.me + n - 2, n)

    def barrier(self):
        sem = pltpu.get_barrier_semaphore()
        for i in range(1, self.n):
            pl.semaphore_signal(sem, inc=1, device_id={'sp': lax.rem(self.me + i, self.n)}, device_id_type=MESH)
        pl.semaphore_wait(sem, self.n - 1)

    def owner(self, delta, base=None):
        return lax.rem((self.me if base is None else base) + 2 * delta, self.n)

    def copy(self, delta, j, send_sem, recv_sem, target):
        piece = self.piece(self.owner(delta), j)
        return pltpu.make_async_remote_copy(src_ref=piece, dst_ref=piece, send_sem=send_sem, recv_sem=recv_sem,
                                            device_id={'sp': target}, device_id_type=MESH)

    def up_copy(self, dist, j):
        delta = lax.rem(self.len - dist, self.len)
        return self.copy(delta, j, self.up_send.at[dist, j], self.ring_recv.at[lax.rem(delta + self.len - 1, self.len), j], self.up)

    def down_copy(self, dist, j):
        return self.copy(dist, j, self.down_send.at[dist, j], self.ring_recv.at[dist + 1, j], self.down)

    def mate_copy(self, delta, j):
        return self.copy(delta, j, self.mate_send.at[delta, j], self.mate_recv.at[delta, j], self.mate)

    def wait_ring(self, delta, j):
        self.copy(delta, j, self.mate_send.at[delta, j], self.ring_recv.at[delta, j], self.mate).wait_recv()

    def wait_mate(self, delta, j):
        piece = self.piece(self.owner(delta, self.mate), j)
        pltpu.make_async_remote_copy(src_ref=piece, dst_ref=piece, send_sem=self.mate_send.at[delta, j], recv_sem=self.mate_recv.at[delta, j],
                                     device_id={'sp': self.mate}, device_id_type=MESH).wait_recv()

    def send_own(self, j):
        self.up_copy(0, j).start()
        self.down_copy(0, j).start()
        self.mate_copy(0, j).start()

    def step(self, r):
        dist, j = r // self.chunks + 1, lax.rem(r, self.chunks)
        last = 2 * self.chunks
        self.wait_ring(self.len - dist, j)

        @pl.when(r < last + self.half)
        def _():
            self.up_copy(dist, j).start()

        self.mate_copy(self.len - dist, j).start()
        self.wait_ring(dist, j)

        @pl.when((r < last) | (r >= last + self.half))
        def _():
            self.down_copy(dist, j).start()

        self.mate_copy(dist, j).start()

    def far_step(self, i):
        far = self.len // 2
        for j in (i, i + self.half):
            self.wait_ring(far, j)
            self.mate_copy(far, j).start()

    def drain(self):
        far = self.len // 2

        @pl.loop(0, self.chunks)
        def _(j):
            for dist in range(far):
                @pl.when((dist < far - 1) | (j < self.half))
                def _(dist=dist):
                    self.up_copy(dist, j).wait_send()

                @pl.when((dist < far - 1) | (j >= self.half))
                def _(dist=dist):
                    self.down_copy(dist, j).wait_send()
            for delta in range(self.len):
                self.mate_copy(delta, j).wait_send()


def ring_scratch(n, chunks):
    length, far = n // 2, n // 4
    dma = pltpu.SemaphoreType.DMA
    return [dma((far, chunks)), dma((far, chunks)), dma((length, chunks)), dma((length, chunks)), dma((length, chunks))]


class Tiles:
    def __init__(self, slots, sems, groups):
        self.slots, self.sems, self.groups = slots, sems, groups
        self.depth, self.total = slots.shape[0], groups[-1][0]

    def copy(self, tile, slot):
        return pltpu.make_async_copy(tile, self.slots.at[slot], self.sems.at[slot])

    def start(self, t):
        first = 0
        for end, pick in self.groups:
            @pl.when((t >= first) & (t < end))
            def _(first=first, pick=pick):
                for cond, tile in pick(t - first):
                    if cond is None:
                        self.copy(tile, lax.rem(t, self.depth)).start()
                    else:
                        @pl.when(cond)
                        def _(tile=tile):
                            self.copy(tile, lax.rem(t, self.depth)).start()
            first = end

    def prime(self):
        for t in range(self.depth - 1):
            self.start(jnp.int32(t))

    def take(self, t):
        self.start(t + self.depth - 1)
        slot = lax.rem(t, self.depth)
        self.copy(self.groups[0][1](0)[0][1], slot).wait()
        return self.slots.at[slot]


def columns(j, width):
    return pl.ds(pl.multiple_of(j * width, width), width)


def block_body(n, cap, span, rows, x_ref, ids_ref, wk_ref, wv_ref, wq_ref, wr_ref, wo_ref, wg_ref, wu_ref, wd_ref, y_ref, e_ref,
               buf, q_ref, row_ref, slots, router_ref, m_ref, l_ref, acc_ref, bias_ref, table_out, table_in,
               sems, router_sem, table_send, table_recv, *ring_sems):
    f32, bf16 = jnp.float32, jnp.bfloat16
    chunks, tok, width = buf.shape[1:]
    depth = slots.shape[1]
    n_exp = router_ref.shape[1]
    n_loc = n_exp // n
    kv_heads = width // HEAD_DIM
    q_tiles = q_ref.shape[1] // width
    parts = q_ref.shape[1] // depth
    act_ref = q_ref.at[:, :depth]

    def kv_piece(src, j):
        return e_ref.at[lax.rem(src, n_loc), columns(src // n_loc, tok), columns(j, width)]

    kv_ring = Ring(n, kv_piece, *ring_sems[:5])
    ring = Ring(n, lambda src, j: buf.at[src, j], *ring_sems[5:])
    me = ring.me
    ends = [1, 2, 2 + q_tiles, 2 + q_tiles + parts * chunks, 2 + q_tiles + (parts + 2) * chunks, 2 + q_tiles + (parts + 3) * chunks]
    tiles = Tiles(slots, sems, (
        (ends[0], lambda t: [(None, wk_ref)]),
        (ends[1], lambda t: [(None, wv_ref)]),
        (ends[2], lambda t: [(None, wq_ref.at[:, columns(t, width)])]),
        (ends[3], lambda t: [(None, wo_ref.at[columns(lax.rem(t, parts), depth), columns(t // parts, width)])]),
        (ends[4], lambda t: [(lax.rem(t, 2) == 0, wg_ref.at[:, columns(t // 2, width)]),
                             (lax.rem(t, 2) == 1, wu_ref.at[:, columns(t // 2, width)])]),
        (ends[5], lambda t: [(None, wd_ref.at[:, columns(t, width)])]),
    ))
    tiles.prime()
    router_copy = pltpu.make_async_copy(wr_ref, router_ref, router_sem.at[0])
    router_copy.start()
    ring.barrier()

    for c in range(2):
        part = jnp.dot(x_ref[...], tiles.take(jnp.int32(c))[...], preferred_element_type=f32).astype(bf16)
        e_ref[lax.rem(me, n_loc), columns(me // n_loc, tok), c * width:(c + 1) * width] = part
        kv_ring.send_own(jnp.int32(c))

    kv_steps = 3 * kv_ring.chunks

    @pl.loop(0, q_tiles)
    def _(j):
        q_ref[:, columns(j, width)] = jnp.dot(x_ref[...], tiles.take(j + 2)[...], preferred_element_type=f32).astype(bf16)

        @pl.when((lax.rem(j, 2) == 1) & (j >= 3) & (j < 3 + 2 * kv_steps))
        def _():
            kv_ring.step((j - 3) // 2)

    for r in range((q_tiles - 2) // 2, kv_steps):
        kv_ring.step(jnp.int32(r))
    far = n // 4
    for delta in range(kv_ring.len):
        if delta != far:
            for c in range(2):
                kv_ring.wait_mate(delta, c)

    per = rows // tok
    heads = q_ref.shape[1] // (kv_heads * HEAD_DIM)
    groups = heads // per
    blocks = span // tok
    halves = n_loc // blocks
    factor = math.log2(math.e) / math.sqrt(HEAD_DIM)
    full = (me * tok) // span
    lanes = [slice(i * 128, (i + 1) * 128) for i in range(span // 128)]
    pos = me * tok - full * span + lax.broadcasted_iota(jnp.int32, bias_ref.shape, 0)
    bias_ref[...] = jnp.where(lax.broadcasted_iota(jnp.int32, bias_ref.shape, 1) <= pos, 0.0, -jnp.inf)

    def head_columns(i, h):
        return columns(i * heads + h, HEAD_DIM)

    def key_block(c, col):
        return e_ref[pl.ds(lax.rem(c, halves) * blocks, blocks), columns(c // halves, tok), columns(col, HEAD_DIM)].reshape(span, HEAD_DIM)

    def attend(i, c, first):
        keys = key_block(c, i)
        vals = key_block(c, kv_heads + i)

        def score(g):
            q = jnp.concatenate([q_ref[:, head_columns(i, g * per + h)] for h in range(per)], axis=0)
            return lax.dot_general(q, keys, NT, preferred_element_type=f32)

        ahead = score(0)
        for g in range(groups):
            s = ahead
            if g + 1 < groups:
                ahead = score(g + 1)
            s = [s[:, k] * factor for k in lanes]
            sl = pl.ds(g * rows, rows)
            if first:
                s = [(x.reshape(per, tok, 128) + bias_ref[:, k][None]).reshape(rows, 128) for x, k in zip(s, lanes)]
            m_new = jnp.max(functools.reduce(jnp.maximum, s), axis=1, keepdims=True)
            if first:
                m_new = jnp.broadcast_to(m_new, (rows, 128))
            else:
                m_old = m_ref[sl, :]
                m_new = jnp.maximum(m_old, m_new)
                alpha = jnp.exp2(m_old - m_new)
            m_ref[sl, :] = m_new
            p = [jnp.exp2(x - m_new) for x in s]
            total = functools.reduce(jnp.add, p)
            out = jnp.dot(jnp.concatenate([x.astype(bf16) for x in p], axis=1), vals, preferred_element_type=f32)
            l_ref[sl, :] = total if first else l_ref[sl, :] * alpha + total
            acc_ref[sl, :] = out if first else acc_ref[sl, :] * alpha + out

    last = jnp.maximum(full - 2 * far // blocks, 0)

    def far_keys():
        kv_ring.far_step(jnp.int32(0))
        for c in range(2):
            kv_ring.wait_mate(far, c)

    @pl.loop(0, kv_heads)
    def _(i):
        attend(i, full, True)

        @pl.loop(0, full)
        def _(k):
            @pl.when((i == 0) & (k == full - 1))
            def _():
                far_keys()

            attend(i, jnp.where(k == full - 1, last, jnp.where(k < last, k, k + 1)), False)

        @pl.when((i == 0) & (full == 0))
        def _():
            far_keys()

        for h in range(heads):
            sl = pl.ds(h * tok, tok)
            total = jnp.sum(l_ref[sl, :], axis=1, keepdims=True)
            q_ref[:, head_columns(i, h)] = (acc_ref[sl, :] * (1.0 / total)).astype(bf16)

    @pl.loop(0, chunks)
    def _(j):
        part = None
        for i in range(parts):
            prod = jnp.dot(q_ref[:, i * depth:(i + 1) * depth], tiles.take(ends[2] + parts * j + i)[...], preferred_element_type=f32)
            part = prod if part is None else part + prod
        h = (x_ref[:, columns(j, width)].astype(f32) + part).astype(bf16)
        buf[me, j] = h
        row_ref[:, columns(j, width)] = h
        ring.send_own(j)

    router_copy.wait()
    expert = lax.broadcasted_iota(jnp.int32, (n_exp, tok), 0)
    chosen = functools.reduce(jnp.logical_or, [ids_ref[c:c + 1, :] == expert for c in range(ids_ref.shape[0])])
    earlier = lax.broadcasted_iota(jnp.int32, (tok, tok), 0) < lax.broadcasted_iota(jnp.int32, (tok, tok), 1)
    count = jnp.dot(jnp.where(chosen, 1.0, 0.0).astype(bf16), jnp.where(earlier, 1.0, 0.0).astype(bf16), preferred_element_type=f32)
    rank = jnp.where(chosen, count, -1.0)
    gate = jax.nn.sigmoid(jnp.dot(row_ref[...], router_ref[...], preferred_element_type=f32)).T
    for d in range(n):
        table_out[d, :n_loc] = rank[d * n_loc:(d + 1) * n_loc]
        table_out[d, n_loc:] = gate[d * n_loc:(d + 1) * n_loc]
    table_in[me] = table_out[me]

    def table_copy(i):
        dst = lax.rem(me + i, n)
        return pltpu.make_async_remote_copy(src_ref=table_out.at[dst], dst_ref=table_in.at[me], send_sem=table_send.at[i], recv_sem=table_recv.at[i],
                                            device_id={'sp': dst}, device_id_type=MESH)

    def table_arrival(i):
        src = lax.rem(me + n - i, n)
        return pltpu.make_async_remote_copy(src_ref=table_out.at[src], dst_ref=table_in.at[src], send_sem=table_send.at[i], recv_sem=table_recv.at[i],
                                            device_id={'sp': src}, device_id_type=MESH)

    for i in range(1, n):
        table_copy(i).start()

    half = chunks // 2

    @pl.loop(0, chunks)
    def _(j):
        h = row_ref[...]
        g = jnp.dot(h, tiles.take(ends[3] + 2 * j)[...], preferred_element_type=f32)
        u = jnp.dot(h, tiles.take(ends[3] + 2 * j + 1)[...], preferred_element_type=f32)
        act_ref[:, columns(j, width)] = (g * jax.nn.sigmoid(g) * u).astype(bf16)
        ring.step(j + jnp.minimum(j, half))

        @pl.when(j < half)
        def _():
            ring.step(2 * j + 1)

    @pl.loop(0, chunks)
    def _(j):
        y = jnp.dot(act_ref[...], tiles.take(ends[4] + j)[...], preferred_element_type=f32)
        y_ref[:, columns(j, width)] = (row_ref[:, columns(j, width)].astype(f32) + y).astype(bf16)

        @pl.when(lax.rem(j, 2) == 1)
        def _():
            ring.step(chunks + half + j // 2)

    kv_ring.drain()
    for i in range(1, n):
        table_arrival(i).wait_recv()

    def expand(src, js):
        shape = (n_loc, cap, tok)
        table = table_in[src]
        place = lax.broadcasted_iota(jnp.int32, shape, 1).astype(f32)
        sel = jnp.where(jnp.broadcast_to(table[:n_loc][:, None, :], shape) == place, 1.0, 0.0)
        scale = jnp.sum(sel * jnp.broadcast_to(table[n_loc:][:, None, :], shape), axis=2, keepdims=True).reshape(n_loc * cap, 1)
        sel = sel.reshape(n_loc * cap, tok).astype(bf16)
        for j in js:
            out = jnp.dot(sel, buf[src, j], preferred_element_type=f32) * scale
            e_ref[:, pl.ds(pl.multiple_of(src * cap, cap), cap), columns(j, width)] = out.astype(bf16).reshape(n_loc, cap, width)

    def expand_pair(delta):
        expand(ring.owner(delta), range(chunks))

        @pl.loop(0, chunks)
        def _(j):
            ring.wait_mate(delta, j)

        expand(ring.owner(delta, ring.mate), range(chunks))

    length = n // 2
    near = 2 * far - 3

    @pl.loop(0, chunks)
    def _(k):
        ring.step(2 * chunks + k)

        @pl.when(k < near)
        def _():
            expand_pair(jnp.where(lax.rem(k, 2) == 1, length - (k + 1) // 2, k // 2))

    def expand_far(i):
        js = (i, i + half)
        expand(ring.owner(far), js)
        for j in js:
            ring.wait_mate(far, j)
        expand(ring.owner(far, ring.mate), js)

    @pl.loop(0, half)
    def _(i):
        ring.far_step(i)

        @pl.when(i < 2)
        def _():
            expand_pair(far + 1 - 2 * i)

        @pl.when(i > 0)
        def _():
            expand_far(i - 1)

    expand_far(jnp.int32(half - 1))
    ring.drain()
    for i in range(1, n):
        table_copy(i).wait_send()


def moe_block(n, cap, tokens, ids, w_key, w_value, w_query, w_router, w_out, w_gate, w_up, w_down, depth=3, span=512, rows=512):
    tok, hidden = tokens.shape
    width = w_key.shape[1]
    q_width = w_query.shape[1]
    chunks = hidden // width
    n_exp = w_router.shape[1]
    n_loc = n_exp // n
    all_rows = tok * q_width // width
    vmem = pl.BlockSpec(memory_space=pltpu.VMEM)
    hbm = pl.BlockSpec(memory_space=pltpu.HBM)
    dma = pltpu.SemaphoreType.DMA
    weights = 2 * w_key.size + w_query.size + w_out.size + w_gate.size + w_up.size + w_down.size
    return pl.pallas_call(
        functools.partial(block_body, n, cap, span, rows),
        out_shape=(pltpu.VMEM((tok, hidden), jnp.bfloat16), pltpu.VMEM((n_loc, n * cap, hidden), jnp.bfloat16)),
        in_specs=[vmem] * 2 + [hbm] * 8,
        out_specs=(vmem, vmem),
        scratch_shapes=[
            pltpu.VMEM((n, chunks, tok, width), jnp.bfloat16),
            pltpu.VMEM((tok, q_width), jnp.bfloat16),
            pltpu.VMEM((tok, hidden), jnp.bfloat16),
            pltpu.VMEM((depth, hidden, width), jnp.bfloat16),
            pltpu.VMEM(w_router.shape, jnp.bfloat16),
            pltpu.VMEM((all_rows, 128), jnp.float32),
            pltpu.VMEM((all_rows, 128), jnp.float32),
            pltpu.VMEM((all_rows, 128), jnp.float32),
            pltpu.VMEM((tok, span), jnp.float32),
            pltpu.VMEM((n, 2 * n_loc, tok), jnp.float32),
            pltpu.VMEM((n, 2 * n_loc, tok), jnp.float32),
            dma((depth,)), dma((1,)), dma((n,)), dma((n,)),
        ] + ring_scratch(n, 2) + ring_scratch(n, chunks),
        cost_estimate=pl.CostEstimate(flops=2 * tok * weights, bytes_accessed=2 * weights, transcendentals=0),
        compiler_params=pltpu.CompilerParams(vmem_limit_bytes=45 * 2 ** 20, collective_id=0, has_side_effects=True),
        name='moe_block',
    )(tokens, ids, w_key, w_value, w_query, w_router, w_out, w_gate, w_up, w_down)


def solution(mesh):
    row_spec = P(('dp', 'sp'), None)
    buf_spec = P(('dp', 'sp'), None, None)
    replicated = P()

    def local_step(tokens, w_query, w_key, w_value, w_out, w_gate, w_up, w_down, w_router, expert_ids):
        tok = tokens.shape[0]
        n_grp = mesh.shape['sp']
        n_experts = w_router.shape[1]
        cap = max(2, (tok * expert_ids.shape[1] // n_experts) * 2)
        hidden_out, expert_buf = moe_block(n_grp, cap, tokens, expert_ids.T, w_key, w_value, w_query, w_router, w_out, w_gate, w_up, w_down)
        return hidden_out, expert_buf

    return jax.shard_map(local_step, mesh=mesh, in_specs=(row_spec,) + (replicated,) * 8 + (row_spec,), out_specs=(row_spec, buf_spec), check_vma=False)
```

```python
import functools
import math
import jax
import jax.numpy as jnp
from jax import lax
from jax.experimental import pallas as pl
from jax.experimental.pallas import tpu as pltpu
from jax.sharding import PartitionSpec as P

HEAD_DIM = 128
NT = (((1,), (1,)), ((), ()))
MESH = pl.DeviceIdType.MESH


class Ring:
    def __init__(self, n, piece, up_send, down_send, ring_recv, mate_send, mate_recv):
        self.n, self.len, self.chunks = n, n // 2, up_send.shape[1]
        self.half = self.chunks // 2
        self.piece, self.up_send, self.down_send = piece, up_send, down_send
        self.ring_recv, self.mate_send, self.mate_recv = ring_recv, mate_send, mate_recv
        self.me = lax.axis_index('sp')
        self.mate = self.me + 1 - 2 * lax.rem(self.me, 2)
        self.up = lax.rem(self.me + 2, n)
        self.down = lax.rem(self.me + n - 2, n)

    def barrier(self):
        sem = pltpu.get_barrier_semaphore()
        for i in range(1, self.n):
            pl.semaphore_signal(sem, inc=1, device_id={'sp': lax.rem(self.me + i, self.n)}, device_id_type=MESH)
        pl.semaphore_wait(sem, self.n - 1)

    def owner(self, delta, base=None):
        return lax.rem((self.me if base is None else base) + 2 * delta, self.n)

    def copy(self, delta, j, send_sem, recv_sem, target):
        piece = self.piece(self.owner(delta), j)
        return pltpu.make_async_remote_copy(src_ref=piece, dst_ref=piece, send_sem=send_sem, recv_sem=recv_sem,
                                            device_id={'sp': target}, device_id_type=MESH)

    def up_copy(self, dist, j):
        delta = lax.rem(self.len - dist, self.len)
        return self.copy(delta, j, self.up_send.at[dist, j], self.ring_recv.at[lax.rem(delta + self.len - 1, self.len), j], self.up)

    def down_copy(self, dist, j):
        return self.copy(dist, j, self.down_send.at[dist, j], self.ring_recv.at[dist + 1, j], self.down)

    def mate_copy(self, delta, j):
        return self.copy(delta, j, self.mate_send.at[delta, j], self.mate_recv.at[delta, j], self.mate)

    def wait_ring(self, delta, j):
        self.copy(delta, j, self.mate_send.at[delta, j], self.ring_recv.at[delta, j], self.mate).wait_recv()

    def wait_mate(self, delta, j):
        piece = self.piece(self.owner(delta, self.mate), j)
        pltpu.make_async_remote_copy(src_ref=piece, dst_ref=piece, send_sem=self.mate_send.at[delta, j], recv_sem=self.mate_recv.at[delta, j],
                                     device_id={'sp': self.mate}, device_id_type=MESH).wait_recv()

    def send_own(self, j):
        self.up_copy(0, j).start()
        self.down_copy(0, j).start()
        self.mate_copy(0, j).start()

    def step(self, r):
        dist, j = r // self.chunks + 1, lax.rem(r, self.chunks)
        last = 2 * self.chunks
        self.wait_ring(self.len - dist, j)

        @pl.when(r < last + self.half)
        def _():
            self.up_copy(dist, j).start()

        self.mate_copy(self.len - dist, j).start()
        self.wait_ring(dist, j)

        @pl.when((r < last) | (r >= last + self.half))
        def _():
            self.down_copy(dist, j).start()

        self.mate_copy(dist, j).start()

    def far_step(self, i):
        far = self.len // 2
        for j in (i, i + self.half):
            self.wait_ring(far, j)
            self.mate_copy(far, j).start()

    def drain(self):
        far = self.len // 2

        @pl.loop(0, self.chunks)
        def _(j):
            for dist in range(far):
                @pl.when((dist < far - 1) | (j < self.half))
                def _(dist=dist):
                    self.up_copy(dist, j).wait_send()

                @pl.when((dist < far - 1) | (j >= self.half))
                def _(dist=dist):
                    self.down_copy(dist, j).wait_send()
            for delta in range(self.len):
                self.mate_copy(delta, j).wait_send()


def ring_scratch(n, chunks):
    length, far = n // 2, n // 4
    dma = pltpu.SemaphoreType.DMA
    return [dma((far, chunks)), dma((far, chunks)), dma((length, chunks)), dma((length, chunks)), dma((length, chunks))]


class Tiles:
    def __init__(self, slots, sems, groups):
        self.slots, self.sems, self.groups = slots, sems, groups
        self.depth, self.total = slots.shape[0], groups[-1][0]

    def copy(self, tile, slot):
        return pltpu.make_async_copy(tile, self.slots.at[slot], self.sems.at[slot])

    def start(self, t):
        first = 0
        for end, pick in self.groups:
            @pl.when((t >= first) & (t < end))
            def _(first=first, pick=pick):
                for cond, tile in pick(t - first):
                    if cond is None:
                        self.copy(tile, lax.rem(t, self.depth)).start()
                    else:
                        @pl.when(cond)
                        def _(tile=tile):
                            self.copy(tile, lax.rem(t, self.depth)).start()
            first = end

    def prime(self):
        for t in range(self.depth - 1):
            self.start(jnp.int32(t))

    def take(self, t):
        self.start(t + self.depth - 1)
        slot = lax.rem(t, self.depth)
        self.copy(self.groups[0][1](0)[0][1], slot).wait()
        return self.slots.at[slot]


def columns(j, width):
    return pl.ds(pl.multiple_of(j * width, width), width)


def block_body(n, cap, span, rows, x_ref, ids_ref, wk_ref, wv_ref, wq_ref, wr_ref, wo_ref, wg_ref, wu_ref, wd_ref, y_ref, e_ref,
               buf, q_ref, row_ref, slots, router_ref, m_ref, l_ref, acc_ref, bias_ref, table_out, table_in,
               x_mate_ref, sems, router_sem, table_send, table_recv, x_sem, q_send, q_recv, *ring_sems):
    f32, bf16 = jnp.float32, jnp.bfloat16
    chunks, tok, width = buf.shape[1:]
    depth = slots.shape[1]
    n_exp = router_ref.shape[1]
    n_loc = n_exp // n
    kv_heads = width // HEAD_DIM
    q_tiles = q_ref.shape[1] // (2 * width)
    core = lax.rem(lax.axis_index('sp'), 2)
    parts = q_ref.shape[1] // depth
    act_ref = q_ref.at[:, :depth]

    def kv_piece(src, j):
        return e_ref.at[lax.rem(src, n_loc), columns(src // n_loc, tok), columns(j, width)]

    kv_ring = Ring(n, kv_piece, *ring_sems[:5])
    ring = Ring(n, lambda src, j: buf.at[src, j], *ring_sems[5:])
    me = ring.me
    ends = [1, 2, 2 + q_tiles, 2 + q_tiles + parts * chunks, 2 + q_tiles + (parts + 2) * chunks, 2 + q_tiles + (parts + 3) * chunks]
    tiles = Tiles(slots, sems, (
        (ends[0], lambda t: [(None, wk_ref)]),
        (ends[1], lambda t: [(None, wv_ref)]),
        (ends[2], lambda t: [(None, wq_ref.at[:, columns(core * q_tiles + t, width)])]),
        (ends[3], lambda t: [(None, wo_ref.at[columns(lax.rem(t, parts), depth), columns(t // parts, width)])]),
        (ends[4], lambda t: [(lax.rem(t, 2) == 0, wg_ref.at[:, columns(t // 2, width)]),
                             (lax.rem(t, 2) == 1, wu_ref.at[:, columns(t // 2, width)])]),
        (ends[5], lambda t: [(None, wd_ref.at[:, columns(t, width)])]),
    ))
    tiles.prime()
    router_copy = pltpu.make_async_copy(wr_ref, router_ref, router_sem.at[0])
    router_copy.start()
    ring.barrier()
    x_copy = pltpu.make_async_remote_copy(src_ref=x_ref, dst_ref=x_mate_ref, send_sem=x_sem.at[0], recv_sem=x_sem.at[1],
                                          device_id={'sp': ring.mate}, device_id_type=MESH)
    x_copy.start()

    for c in range(2):
        part = jnp.dot(x_ref[...], tiles.take(jnp.int32(c))[...], preferred_element_type=f32).astype(bf16)
        e_ref[lax.rem(me, n_loc), columns(me // n_loc, tok), c * width:(c + 1) * width] = part
        kv_ring.send_own(jnp.int32(c))

    kv_steps = 3 * kv_ring.chunks

    def q_copy(j, owner):
        return pltpu.make_async_remote_copy(src_ref=row_ref.at[:, columns(j, width)], dst_ref=q_ref.at[:, columns(owner * q_tiles + j, width)],
                                            send_sem=q_send.at[j], recv_sem=q_recv.at[j], device_id={'sp': ring.mate}, device_id_type=MESH)

    x_copy.wait_recv()

    @pl.loop(0, q_tiles)
    def _(j):
        tile = tiles.take(j + 2)
        row_ref[:, columns(j, width)] = jnp.dot(x_mate_ref[...], tile[...], preferred_element_type=f32).astype(bf16)
        q_copy(j, core).start()
        q_ref[:, columns(core * q_tiles + j, width)] = jnp.dot(x_ref[...], tile[...], preferred_element_type=f32).astype(bf16)

        @pl.when(j >= 2)
        def _():
            kv_ring.step(j - 2)

    far = n // 4
    ready = q_tiles - 2

    def mate_keys(deltas):
        for delta in deltas:
            for c in range(2):
                kv_ring.wait_mate(delta, c)

    mate_keys((0, 1, kv_ring.len - 1))

    @pl.loop(0, q_tiles)
    def _(j):
        q_copy(j, 1 - core).wait_recv()
        q_copy(j, core).wait_send()

    x_copy.wait_send()

    per = rows // tok
    heads = q_ref.shape[1] // (kv_heads * HEAD_DIM)
    groups = heads // per
    blocks = span // tok
    halves = n_loc // blocks
    factor = math.log2(math.e) / math.sqrt(HEAD_DIM)
    full = (me * tok) // span
    lanes = [slice(i * 128, (i + 1) * 128) for i in range(span // 128)]
    pos = me * tok - full * span + lax.broadcasted_iota(jnp.int32, bias_ref.shape, 0)
    bias_ref[...] = jnp.where(lax.broadcasted_iota(jnp.int32, bias_ref.shape, 1) <= pos, 0.0, -jnp.inf)

    def head_columns(i, h):
        return columns(i * heads + h, HEAD_DIM)

    def key_block(c, col):
        return e_ref[pl.ds(lax.rem(c, halves) * blocks, blocks), columns(c // halves, tok), columns(col, HEAD_DIM)].reshape(span, HEAD_DIM)

    def attend(i, c, first):
        keys = key_block(c, i)
        vals = key_block(c, kv_heads + i)

        def score(g):
            q = jnp.concatenate([q_ref[:, head_columns(i, g * per + h)] for h in range(per)], axis=0)
            return lax.dot_general(q, keys, NT, preferred_element_type=f32)

        ahead = score(0)
        for g in range(groups):
            s = ahead
            if g + 1 < groups:
                ahead = score(g + 1)
            s = [s[:, k] * factor for k in lanes]
            sl = pl.ds(g * rows, rows)
            if first:
                s = [(x.reshape(per, tok, 128) + bias_ref[:, k][None]).reshape(rows, 128) for x, k in zip(s, lanes)]
            m_new = jnp.max(functools.reduce(jnp.maximum, s), axis=1, keepdims=True)
            if first:
                m_new = jnp.broadcast_to(m_new, (rows, 128))
            else:
                m_old = m_ref[sl, :]
                m_new = jnp.maximum(m_old, m_new)
                alpha = jnp.exp2(m_old - m_new)
            m_ref[sl, :] = m_new
            p = [jnp.exp2(x - m_new) for x in s]
            total = functools.reduce(jnp.add, p)
            out = jnp.dot(jnp.concatenate([x.astype(bf16) for x in p], axis=1), vals, preferred_element_type=f32)
            l_ref[sl, :] = total if first else l_ref[sl, :] * alpha + total
            acc_ref[sl, :] = out if first else acc_ref[sl, :] * alpha + out

    last = jnp.maximum(full - 2 * far // blocks, 0)

    def far_keys():
        kv_ring.far_step(jnp.int32(0))
        for c in range(2):
            kv_ring.wait_mate(far, c)

    @pl.loop(0, kv_heads)
    def _(i):
        attend(i, full, True)

        @pl.when(i == 0)
        def _():
            for r in range(ready, kv_steps):
                kv_ring.step(jnp.int32(r))
            mate_keys([d for d in range(2, kv_ring.len - 1) if d != far])

        @pl.loop(0, full)
        def _(k):
            @pl.when((i == 0) & (k == full - 1))
            def _():
                far_keys()

            attend(i, jnp.where(k == full - 1, last, jnp.where(k < last, k, k + 1)), False)

        @pl.when((i == 0) & (full == 0))
        def _():
            far_keys()

        for h in range(heads):
            sl = pl.ds(h * tok, tok)
            total = jnp.sum(l_ref[sl, :], axis=1, keepdims=True)
            q_ref[:, head_columns(i, h)] = (acc_ref[sl, :] * (1.0 / total)).astype(bf16)

    @pl.loop(0, chunks)
    def _(j):
        part = None
        for i in range(parts):
            prod = jnp.dot(q_ref[:, i * depth:(i + 1) * depth], tiles.take(ends[2] + parts * j + i)[...], preferred_element_type=f32)
            part = prod if part is None else part + prod
        h = (x_ref[:, columns(j, width)].astype(f32) + part).astype(bf16)
        buf[me, j] = h
        row_ref[:, columns(j, width)] = h
        ring.send_own(j)

        @pl.when(j >= chunks - 2)
        def _():
            ring.step(j - (chunks - 2))

    router_copy.wait()
    expert = lax.broadcasted_iota(jnp.int32, (n_exp, tok), 0)
    chosen = functools.reduce(jnp.logical_or, [ids_ref[c:c + 1, :] == expert for c in range(ids_ref.shape[0])])
    earlier = lax.broadcasted_iota(jnp.int32, (tok, tok), 0) < lax.broadcasted_iota(jnp.int32, (tok, tok), 1)
    count = jnp.dot(jnp.where(chosen, 1.0, 0.0).astype(bf16), jnp.where(earlier, 1.0, 0.0).astype(bf16), preferred_element_type=f32)
    rank = jnp.where(chosen, count, -1.0)
    gate = jax.nn.sigmoid(jnp.dot(row_ref[...], router_ref[...], preferred_element_type=f32)).T
    for d in range(n):
        table_out[d, :n_loc] = rank[d * n_loc:(d + 1) * n_loc]
        table_out[d, n_loc:] = gate[d * n_loc:(d + 1) * n_loc]
    table_in[me] = table_out[me]

    def table_copy(i):
        dst = lax.rem(me + i, n)
        return pltpu.make_async_remote_copy(src_ref=table_out.at[dst], dst_ref=table_in.at[me], send_sem=table_send.at[i], recv_sem=table_recv.at[i],
                                            device_id={'sp': dst}, device_id_type=MESH)

    def table_arrival(i):
        src = lax.rem(me + n - i, n)
        return pltpu.make_async_remote_copy(src_ref=table_out.at[src], dst_ref=table_in.at[src], send_sem=table_send.at[i], recv_sem=table_recv.at[i],
                                            device_id={'sp': src}, device_id_type=MESH)

    for i in range(1, n):
        table_copy(i).start()

    half = chunks // 2

    @pl.loop(0, chunks)
    def _(j):
        h = row_ref[...]
        g = jnp.dot(h, tiles.take(ends[3] + 2 * j)[...], preferred_element_type=f32)
        u = jnp.dot(h, tiles.take(ends[3] + 2 * j + 1)[...], preferred_element_type=f32)
        act_ref[:, columns(j, width)] = (g * jax.nn.sigmoid(g) * u).astype(bf16)
        ring.step(2 + j + jnp.minimum(j, half - 1))

        @pl.when(j < half - 1)
        def _():
            ring.step(2 * j + 3)

    @pl.loop(0, chunks)
    def _(j):
        y = jnp.dot(act_ref[...], tiles.take(ends[4] + j)[...], preferred_element_type=f32)
        y_ref[:, columns(j, width)] = (row_ref[:, columns(j, width)].astype(f32) + y).astype(bf16)

        @pl.when(lax.rem(j, 2) == 1)
        def _():
            ring.step(chunks + half + 1 + j // 2)

    kv_ring.drain()
    for i in range(1, n):
        table_arrival(i).wait_recv()

    def expand(src, js):
        shape = (n_loc, cap, tok)
        table = table_in[src]
        place = lax.broadcasted_iota(jnp.int32, shape, 1).astype(f32)
        sel = jnp.where(jnp.broadcast_to(table[:n_loc][:, None, :], shape) == place, 1.0, 0.0)
        scale = jnp.sum(sel * jnp.broadcast_to(table[n_loc:][:, None, :], shape), axis=2, keepdims=True).reshape(n_loc * cap, 1)
        sel = sel.reshape(n_loc * cap, tok).astype(bf16)
        for j in js:
            out = jnp.dot(sel, buf[src, j], preferred_element_type=f32) * scale
            e_ref[:, pl.ds(pl.multiple_of(src * cap, cap), cap), columns(j, width)] = out.astype(bf16).reshape(n_loc, cap, width)

    def expand_pair(delta):
        expand(ring.owner(delta), range(chunks))

        @pl.loop(0, chunks)
        def _(j):
            ring.wait_mate(delta, j)

        expand(ring.owner(delta, ring.mate), range(chunks))

    length = n // 2
    near = 2 * far - 3

    @pl.loop(0, chunks - 1)
    def _(k):
        ring.step(2 * chunks + 1 + k)

        @pl.when(k < near)
        def _():
            expand_pair(jnp.where(lax.rem(k, 2) == 1, length - (k + 1) // 2, k // 2))

    def expand_far(i):
        js = (i, i + half)
        expand(ring.owner(far), js)
        for j in js:
            ring.wait_mate(far, j)
        expand(ring.owner(far, ring.mate), js)

    @pl.loop(0, half)
    def _(i):
        ring.far_step(i)

        @pl.when(i < 2)
        def _():
            expand_pair(far + 1 - 2 * i)

        @pl.when(i > 0)
        def _():
            expand_far(i - 1)

    expand_far(jnp.int32(half - 1))
    ring.drain()
    for i in range(1, n):
        table_copy(i).wait_send()


def moe_block(n, cap, tokens, ids, w_key, w_value, w_query, w_router, w_out, w_gate, w_up, w_down, depth=3, span=512, rows=512):
    tok, hidden = tokens.shape
    width = w_key.shape[1]
    q_width = w_query.shape[1]
    chunks = hidden // width
    n_exp = w_router.shape[1]
    n_loc = n_exp // n
    all_rows = tok * q_width // width
    half_tiles = q_width // (2 * width)
    vmem = pl.BlockSpec(memory_space=pltpu.VMEM)
    hbm = pl.BlockSpec(memory_space=pltpu.HBM)
    dma = pltpu.SemaphoreType.DMA
    weights = 2 * w_key.size + w_query.size + w_out.size + w_gate.size + w_up.size + w_down.size
    return pl.pallas_call(
        functools.partial(block_body, n, cap, span, rows),
        out_shape=(pltpu.VMEM((tok, hidden), jnp.bfloat16), pltpu.VMEM((n_loc, n * cap, hidden), jnp.bfloat16)),
        in_specs=[vmem] * 2 + [hbm] * 8,
        out_specs=(vmem, vmem),
        scratch_shapes=[
            pltpu.VMEM((n, chunks, tok, width), jnp.bfloat16),
            pltpu.VMEM((tok, q_width), jnp.bfloat16),
            pltpu.VMEM((tok, hidden), jnp.bfloat16),
            pltpu.VMEM((depth, hidden, width), jnp.bfloat16),
            pltpu.VMEM(w_router.shape, jnp.bfloat16),
            pltpu.VMEM((all_rows, 128), jnp.float32),
            pltpu.VMEM((all_rows, 128), jnp.float32),
            pltpu.VMEM((all_rows, 128), jnp.float32),
            pltpu.VMEM((tok, span), jnp.float32),
            pltpu.VMEM((n, 2 * n_loc, tok), jnp.float32),
            pltpu.VMEM((n, 2 * n_loc, tok), jnp.float32),
            pltpu.VMEM((tok, hidden), jnp.bfloat16),
            dma((depth,)), dma((1,)), dma((n,)), dma((n,)), dma((2,)), dma((half_tiles,)), dma((half_tiles,)),
        ] + ring_scratch(n, 2) + ring_scratch(n, chunks),
        cost_estimate=pl.CostEstimate(flops=2 * tok * weights, bytes_accessed=2 * weights, transcendentals=0),
        compiler_params=pltpu.CompilerParams(vmem_limit_bytes=46 * 2 ** 20, collective_id=0, has_side_effects=True),
        name='moe_block',
    )(tokens, ids, w_key, w_value, w_query, w_router, w_out, w_gate, w_up, w_down)


def solution(mesh):
    row_spec = P(('dp', 'sp'), None)
    buf_spec = P(('dp', 'sp'), None, None)
    replicated = P()

    def local_step(tokens, w_query, w_key, w_value, w_out, w_gate, w_up, w_down, w_router, expert_ids):
        tok = tokens.shape[0]
        n_grp = mesh.shape['sp']
        n_experts = w_router.shape[1]
        cap = max(2, (tok * expert_ids.shape[1] // n_experts) * 2)
        hidden_out, expert_buf = moe_block(n_grp, cap, tokens, expert_ids.T, w_key, w_value, w_query, w_router, w_out, w_gate, w_up, w_down)
        return hidden_out, expert_buf

    return jax.shard_map(local_step, mesh=mesh, in_specs=(row_spec,) + (replicated,) * 8 + (row_spec,), out_specs=(row_spec, buf_spec), check_vma=False)
```
